128 devices in a mesh: dp: 8 (over y, core), tensor: 16 (over x, z).
Axes of the slice: x: 4, y: 4, z: 4, core: 2. Of those that a mesh axis runs over, the one named last changes fastest.
Arguments:
- inputs: bfloat16 [24576, 5120], P('dp', 'tensor'), may hold values from -6 to 6
- cotangent: bfloat16 [24576, 4096], P('dp', 'tensor'), may hold values from -192 to 192
- lengths: int32 [64], P('dp'), may hold values from 96 to 384
- momentum: float32 [8, 4096, 5120], P('dp', 'tensor'), may hold values from -26 to 26
- weight: bfloat16 [4096, 5120], P('tensor'), may hold values from -0.00039863586 to 0.00039863586
- right_factor: float32 [5120, 64], replicated, may hold values from -1 to 1
Outputs:
- new_weight: bfloat16 [4096, 5120], P('tensor')
- new_momentum: float32 [8, 4096, 5120], P('dp', 'tensor')
- new_right: float32 [5120, 64], replicated
The draws below stay inside these ranges and needn't reach their ends.
Inputs may be any that keep to these rules, and one draw needn't show every extreme that they name: The first lengths[i] positions of block i are real tokens, the rest padding.
All inputs are finite; a program needn't handle non-finite values.
Results may differ from the reference program's by a relative error of at most 0.00045.
Values may be sent and summed in bfloat16 or wider, within the bound.
A program may use at most 128 MiB of HBM per device.

```python
import math
import jax
import jax.numpy as jnp
from jax import lax

ROWS = 4096
COLS = 5120
RANK = 64
BLOCK = 384
BLOCKS = 8
REPLICAS = 8
TOKENS = 24576
ALL_BLOCKS = 64
N_DP = 8


def shared_factors(key):
    left_basis = jax.random.truncated_normal(jax.random.fold_in(key, 101), -4.0, 4.0, (ROWS, RANK), jnp.float32)
    right_basis = jax.random.truncated_normal(jax.random.fold_in(key, 102), -4.0, 4.0, (COLS, RANK), jnp.float32)
    return (left_basis, right_basis)


def draw_momentum(key, part):
    left_basis, right_basis = shared_factors(key)
    spread = math.log(3.0)
    jitter = jax.random.truncated_normal(jax.random.fold_in(key, 104), -6.0, 6.0, (REPLICAS, ROWS, COLS), jnp.float32)
    scales = jnp.exp(jax.random.uniform(jax.random.fold_in(key, 103), (RANK,), jnp.float32) * spread)
    amplitude = 2.5 / jnp.sqrt(jnp.sum(scales * scales))
    common = jnp.dot(left_basis * (scales * amplitude)[None, :], right_basis.T, precision=lax.Precision.HIGHEST)
    common = jnp.clip(common, -20.0, 20.0)
    return common[None] + jitter


def draw_right_factor(key, part):
    left_basis, right_basis = shared_factors(key)
    columns = right_basis / jnp.sqrt(jnp.sum(right_basis * right_basis, axis=0))[None, :]
    jitter = jax.random.truncated_normal(jax.random.fold_in(key, 201), -4.0, 4.0, (COLS, RANK), jnp.float32)
    return jnp.clip(columns + jitter * (0.5 / math.sqrt(COLS)), -1.0, 1.0)


def touch_ends(values, key, low, top_value):
    dims = values.shape
    spot = [jax.random.randint(jax.random.fold_in(key, axis), (), 0, dims[axis]) for axis in range(len(dims))]
    values = values.at[tuple(spot)].set(low)
    longest = dims.index(max(dims))
    spot[longest] = (spot[longest] + 1) % dims[longest]
    return values.at[tuple(spot)].set(top_value)


def steps_of(key, extent, cuts, least, largest):
    loudness, own = 1.0, jax.random.fold_in(key, 6)
    for dim, parts in cuts:
        heights = jnp.exp(jax.random.uniform(jax.random.fold_in(own, dim), (parts,), jnp.float32, least / len(cuts), largest / len(cuts)))
        loudness = loudness * jnp.repeat(heights, extent[dim] // parts).reshape([-1 if axis == dim else 1 for axis in range(len(extent))])
    return loudness


def centred(rng, extent, deviation, bound, cuts=(), held_as=jnp.bfloat16):
    values = deviation * jax.random.normal(rng, extent, jnp.float32)
    if cuts:
        values = values * steps_of(rng, extent, cuts, -0.22, 0.18)
    return jnp.clip(values, -bound, bound).astype(held_as)


def setup_inputs(seed: int = 0) -> dict:
    arg_keys = jax.random.split(jax.random.key(seed), 7)
    return {
        "inputs": centred(arg_keys[0], (TOKENS, COLS), 1.0, 6.0, ((0, 8), (1, 16))),
        "cotangent": centred(arg_keys[1], (TOKENS, ROWS), 32.0, 192.0, ((0, 8), (1, 16))),
        "lengths": touch_ends(jax.random.randint(arg_keys[2], (ALL_BLOCKS,), BLOCK // 4, BLOCK + 1), jax.random.fold_in(arg_keys[2], 1), BLOCK // 4, BLOCK).astype(jnp.int32),
        "momentum": draw_momentum(jax.random.fold_in(arg_keys[6], 71), 0),
        "weight": centred(arg_keys[4], (ROWS, COLS), 0.00006, 0.00039863586, ((0, 16),)),
        "right_factor": draw_right_factor(jax.random.fold_in(arg_keys[6], 71), 0),
    }


EPS = 1e-06
MU = 0.95
LR = 0.02

def reference(inputs, cotangent, lengths, momentum, weight, right_factor):
    hi = lax.Precision.HIGHEST
    per = BLOCKS * BLOCK
    position = jnp.arange(BLOCK, dtype=jnp.int32)
    keep = (position[None, :] < lengths[:, None]).reshape(-1).astype(jnp.bfloat16)
    masked = inputs * keep[:, None]
    counts = lax.optimization_barrier(jnp.sum(lengths.reshape(N_DP, BLOCKS).astype(jnp.float32), axis=1))
    boths = []
    total = jnp.zeros((ROWS, RANK), jnp.float32)
    for replica in range(N_DP):
        lower = replica * per
        grad = lax.dot_general(cotangent[lower:lower + per].astype(jnp.float32), masked[lower:lower + per].astype(jnp.float32), (((0,), (0,)), ((), ())), preferred_element_type=jnp.float32)
        both = momentum[replica] + grad / counts[replica]
        boths.append(both)
        total = total + jnp.dot(both, right_factor, precision=hi)
    left = total / N_DP
    gram = jnp.dot(left.T, left, precision=hi)
    factor = jnp.linalg.cholesky(gram)
    ortho = jax.scipy.linalg.solve_triangular(factor, left.T, lower=True).T
    right = jnp.zeros((COLS, RANK), jnp.float32)
    for replica in range(N_DP):
        right = right + lax.dot_general(boths[replica], ortho, (((0,), (0,)), ((), ())), precision=hi) / N_DP
    new_right = right * lax.rsqrt(lax.optimization_barrier(jnp.sum(right * right, axis=0)) + EPS)
    lowrank = jnp.dot(ortho, right.T, precision=hi)
    new_momentum = jnp.stack([both - (1.0 - MU) * lowrank for both in boths])
    update = jnp.dot(ortho, new_right.T, precision=hi)
    new_weight = (weight.astype(jnp.float32) - LR * math.sqrt(ROWS / COLS) * update).astype(jnp.bfloat16)
    return (new_weight, new_momentum, new_right)
```

```python
import functools
import math

import jax
import jax.numpy as jnp
from jax import lax
from jax.experimental import pallas as pl
from jax.experimental.pallas import tpu as pltpu
from jax.sharding import PartitionSpec as P

EPS = 1e-06
MU = 0.95
LR = 0.02

f32 = jnp.float32
bf16 = jnp.bfloat16
HI = lax.Precision.HIGHEST
VMEM = pltpu.VMEM
DMA = pltpu.SemaphoreType.DMA
CODES = 32767.0


def vspec():
    return pl.BlockSpec(memory_space=pltpu.VMEM)


def anyspec():
    return pl.BlockSpec(memory_space=pl.ANY)


def tensor_place():
    t = lax.axis_index("tensor")
    return lax.div(t, 4), lax.rem(t, 4)


def around(i, by):
    return lax.rem(i + by, 4)


def remote(src, dst, send, recv, where):
    return pltpu.make_async_remote_copy(
        src_ref=src,
        dst_ref=dst,
        send_sem=send,
        recv_sem=recv,
        device_id=where,
        device_id_type=pl.DeviceIdType.MESH,
    )


def greet(peers):
    barrier = pltpu.get_barrier_semaphore()
    for peer in peers:
        pl.semaphore_signal(barrier, inc=1, device_id=peer, device_id_type=pl.DeviceIdType.MESH)
    pl.semaphore_wait(barrier, len(peers))


def grad_kernel(
    cot, packed, inv, mom, rf, both, left_t,
    A, B, codes, scales, R, RS, p1, p2, rfv, left, sl, sa, ra, sb, rb, sc, ss, rc, rs,
):
    x, z = tensor_place()
    zl, zr, zo = around(z, 3), around(z, 1), around(z, 2)
    xl, xr, xo = around(x, 3), around(x, 1), around(x, 2)

    def at(xx, zz):
        return {"tensor": xx * 4 + zz}

    tok = cot.shape[0]
    ha, hb = tok // 2, packed.shape[0] // 2
    width = packed.shape[1] // 2
    rows = cot.shape[1]

    locals_ = [
        pltpu.make_async_copy(cot, A.at[z], sl.at[0]),
        pltpu.make_async_copy(packed, B.at[x], sl.at[1]),
        pltpu.make_async_copy(mom, both, sl.at[2]),
        pltpu.make_async_copy(rf, rfv, sl.at[3]),
    ]
    greet([at(x, zl), at(x, zr), at(x, zo), at(xl, z), at(xr, z)])

    def part_a(h):
        return pl.ds(h * ha, ha)

    def part_b(h):
        return pl.ds(h * hb, hb)

    sent = []
    for half, right in ((0, True), (1, False), (1, True), (0, False)):
        k = half + (0 if right else 2)
        ca = remote(cot.at[part_a(half)], A.at[z, part_a(half)], sa.at[k], ra.at[k], at(x, zr if right else zl))
        ca.start()
        cb = remote(packed.at[part_b(half)], B.at[x, part_b(half)], sb.at[k], rb.at[k], at(xr if right else xl, z))
        cb.start()
        sent += [ca, cb]
    for c in locals_:
        c.start()

    def got_a(k):
        remote(A.at[z, part_a(0)], A.at[z, part_a(0)], sa.at[k], ra.at[k], at(x, zr)).wait_recv()

    def got_b(k):
        remote(B.at[x, part_b(0)], B.at[x, part_b(0)], sb.at[0], rb.at[k], at(xr, z)).wait_recv()

    def pass_a(k, half, origin, to):
        c = remote(A.at[origin, part_a(half)], A.at[origin, part_a(half)], sa.at[k], ra.at[k], at(x, to))
        c.start()
        sent.append(c)

    def pass_b(k, half, origin, to):
        c = remote(B.at[origin, part_b(half)], B.at[origin, part_b(half)], sb.at[k], rb.at[k], at(to, z))
        c.start()
        sent.append(c)

    got_a(0)
    pass_a(4, 0, zl, zr)
    got_a(3)
    pass_a(5, 1, zr, zl)
    got_b(0)
    pass_b(4, 0, xl, xr)
    got_b(3)
    pass_b(5, 1, xr, xl)

    pair0 = lax.div(x, 2)
    odd = lax.rem(x, 2)
    scale_in = inv[0]
    depth = 256

    def unit(i, carry):
        j, s = lax.div(i, 4), lax.rem(i, 4)
        ends = jnp.where(s == 0, 0, 2)
        ends = jnp.where(j == 0, ends, 2 - ends)
        off = jnp.where(s == 1, 3, jnp.where(s == 2, 1, ends))
        zz = around(z, off)
        pair = jnp.where(j == 0, pair0, 1 - pair0)

        @pl.when(i == 0)
        def _():
            locals_[0].wait()
            locals_[1].wait()
            got_b(2 - odd)

        @pl.when(i == 1)
        def _():
            got_a(1)

        @pl.when(i == 2)
        def _():
            got_a(2)

        @pl.when(i == 3)
        def _():
            got_a(4)
            got_a(5)

        @pl.when(i == 4)
        def _():
            got_b(1 + odd)
            got_b(4)
            got_b(5)

        p1[...] = jnp.zeros_like(p1)
        p2[...] = jnp.zeros_like(p2)

        def step(k, c):
            low = pl.ds(pl.multiple_of(k * depth, depth), depth)
            high = pl.ds(pl.multiple_of(ha + k * depth, depth), depth)
            a_low = A[zz, low, :]
            a_high = A[zz, high, :]
            for e in range(2):
                xx = pair * 2 + e
                p1[e] += lax.dot_general(
                    a_low, B[xx, low, 0:384], (((0,), (0,)), ((), ())), preferred_element_type=f32
                )
                p2[e] += lax.dot_general(
                    a_high, B[xx, low, 256:640], (((0,), (0,)), ((), ())), preferred_element_type=f32
                )
            return c

        lax.fori_loop(0, ha // depth, step, 0)
        p1[0] = p1[0] + pltpu.roll(p2[0], 384 - 64, 1)
        p1[1] = p2[1] + pltpu.roll(p1[1], 64, 1)
        low_lane = lax.broadcasted_iota(jnp.int32, (rows, 128), 1) < 64
        own = off == 0
        parts = (
            (0, 256, lambda: p1[0, :, 0:256]),
            (256, 128, lambda: jnp.where(low_lane, p1[0, :, 256:384], p1[1, :, 0:128])),
            (384, 256, lambda: p1[1, :, 128:384]),
        )
        for start, size, value in parts:
            v = value() * scale_in
            top = jnp.max(jnp.abs(v), axis=0, keepdims=True)
            live = top > 1e-30
            code = jnp.round(v * jnp.where(live, CODES / jnp.where(live, top, 1.0), 0.0))
            code = code.astype(jnp.int32).astype(jnp.int16)
            back = jnp.broadcast_to(jnp.where(live, top, 0.0) * (1.0 / CODES), (8, size))
            lanes = slice(start, start + size)

            @pl.when(own)
            def _():
                R[pair, z, :, lanes] = code
                RS[pair, z, :, lanes] = back

            @pl.when(jnp.logical_not(own))
            def _():
                codes[i, :, lanes] = code
                scales[i, :, lanes] = back

        @pl.when(jnp.logical_not(own))
        def _():
            remote(codes.at[i], R.at[pair, z], sc.at[i], rc.at[pair, z], at(x, zz)).start()
            remote(scales.at[i], RS.at[pair, z], ss.at[i], rs.at[pair, z], at(x, zz)).start()

        return carry

    lax.fori_loop(0, 8, unit, 0)
    locals_[2].wait()
    locals_[3].wait()
    left[...] = jnp.zeros_like(left)
    low_lane = lax.broadcasted_iota(jnp.int32, (64, 128), 1) < 64
    for j in range(2):
        pair = pair0 if j == 0 else 1 - pair0
        for by in (1, 3, 2):
            zz = around(z, by)
            remote(codes.at[0], R.at[pair, zz], sc.at[0], rc.at[pair, zz], at(x, zz)).wait_recv()
            remote(scales.at[0], RS.at[pair, zz], ss.at[0], rs.at[pair, zz], at(x, zz)).wait_recv()
        for e in range(2):
            for h in range(2):
                base = pl.multiple_of((pair * 2 + e) * 4 * width + h * 2 * width, 640)

                def piece(zz, r):
                    lanes = slice(0, 384) if e == 0 else slice(256, 640)
                    v = R[pair, zz, r, lanes].astype(jnp.int32).astype(f32) * RS[pair, zz, 0:1, lanes]
                    if zz % 2 == 0 and e == 1:
                        v = pltpu.roll(v, 384 - 64, 1)
                    if zz % 2 == 1 and e == 0:
                        v = pltpu.roll(v, 64, 1)
                    return v

                def chunk(q, c):
                    r = pl.ds(pl.multiple_of(q * 64, 64), 64)
                    first, second = piece(2 * h, r), piece(2 * h + 1, r)
                    both[r, pl.ds(base, 256)] += first[:, 0:256]
                    both[r, pl.ds(pl.multiple_of(base + 256, 128), 128)] += jnp.where(
                        low_lane, first[:, 256:384], second[:, 0:128]
                    )
                    both[r, pl.ds(pl.multiple_of(base + 384, 128), 256)] += second[:, 128:384]
                    return c

                lax.fori_loop(0, rows // 64, chunk, 0)
                left[...] += jnp.dot(
                    both[:, pl.ds(base, 640)], rfv[pl.ds(base, 640), :], precision=HI, preferred_element_type=f32
                )
    left_t[...] = left[...].T
    for c in sent:
        c.wait_send()
    for i in range(1, 7):
        remote(codes.at[i], R.at[0, 0], sc.at[i], rc.at[0, 0], at(x, zr)).wait_send()
        remote(scales.at[i], RS.at[0, 0], ss.at[i], rs.at[0, 0], at(x, zr)).wait_send()


def gradient(cot, packed, inv, mom, rf):
    tok, rows = cot.shape
    cols = mom.shape[1]
    rank = rf.shape[1]
    return pl.pallas_call(
        grad_kernel,
        out_shape=(
            jax.ShapeDtypeStruct((rows, cols), f32),
            jax.ShapeDtypeStruct((rank, rows), f32),
        ),
        in_specs=[anyspec(), anyspec(), pl.BlockSpec(memory_space=pltpu.SMEM), anyspec(), anyspec()],
        out_specs=(vspec(), vspec()),
        scratch_shapes=[
            VMEM((4, tok, rows), bf16),
            VMEM((4,) + packed.shape, bf16),
            VMEM((8, rows, 640), jnp.int16),
            VMEM((8, 8, 640), f32),
            VMEM((2, 4, rows, 640), jnp.int16),
            VMEM((2, 4, 8, 640), f32),
            VMEM((2, rows, 384), f32),
            VMEM((2, rows, 384), f32),
            VMEM((cols, rank), f32),
            VMEM((rows, rank), f32),
            DMA((4,)), DMA((6,)), DMA((6,)), DMA((6,)), DMA((6,)),
            DMA((8,)), DMA((8,)), DMA((2, 4)), DMA((2, 4)),
        ],
        compiler_params=pltpu.CompilerParams(collective_id=0, has_side_effects=True),
        name="grad2d",
    )(cot, packed, inv, mom, rf)


def sums_kernel(
    part, both, out, left_out, gram_out,
    L0, L1, T, D, P1, P2, P3, G1, G2, send, recv,
):
    x, z = tensor_place()
    d = lax.axis_index("dp")
    y, c = lax.div(d, 2), lax.rem(d, 2)
    place = {"x": x, "y": y, "z": z}

    def at(axis, k):
        if axis == "core":
            return {"dp": y * 2 + k}
        if axis == "y":
            return {"dp": k * 2 + c}
        if axis == "x":
            return {"tensor": k * 4 + z}
        return {"tensor": x * 4 + k}

    mate = at("core", 1 - c)
    greet([mate] + [at(a, around(place[a], q)) for a in "xyz" for q in (1, 2, 3)])
    pending = []

    def swap(stage, src, dst):
        copy = remote(src, dst, send.at[stage, 0], recv.at[stage, 0], mate)
        copy.start()
        pending.append(copy)
        return copy

    def spread(stage, axis, src, dst):
        me = place[axis]
        waits = []
        for q in (2, 1, 3):
            k = around(me, q)
            copy = remote(src(k), dst(me), send.at[stage, q], recv.at[stage, q], at(axis, k))
            copy.start()
            pending.append(copy)
            waits.append(remote(src(k), dst(around(me, 4 - q)), send.at[stage, q], recv.at[stage, q], at(axis, k)))

        def wait():
            for w in waits:
                w.wait_recv()

        return wait

    swap(0, part, L0).wait_recv()
    L1[y] = part[...] + L0[...]
    spread(1, "y", lambda k: L1.at[y], lambda k: L1.at[k])()
    left = (L1[0] + L1[1] + L1[2] + L1[3]) * (1.0 / 8.0)
    left_out[...] = left
    gram = lax.dot_general(left, left, (((1,), (1,)), ((), ())), precision=HI, preferred_element_type=f32)
    G1[z] = gram
    gram_wait = spread(2, "z", lambda k: G1.at[z], lambda k: G1.at[k])

    tiles = both.shape[1] // 128
    half = tiles * 8 // 2

    def block(g, carry):
        cols = pl.ds(pl.multiple_of(g * 640, 640), 640)
        v = jnp.dot(left_out[...], both[:, cols], precision=HI, preferred_element_type=f32)
        for i in range(5):
            T[pl.ds(g * 40 + i * 8, 8)] = v[:, 128 * i : 128 * (i + 1)].reshape(8, 8, 128)
        return carry

    lax.fori_loop(4 * (1 - c), 4 * (1 - c) + 4, block, 0)
    mine, theirs = c * half, (1 - c) * half
    core_wait = swap(3, T.at[pl.ds(theirs, half)], D)
    lax.fori_loop(4 * c, 4 * c + 4, block, 0)
    core_wait.wait_recv()

    def add_core(g, carry):
        r = pl.ds(mine + g * 20, 20)
        T[r] = T[r] + D[pl.ds(g * 20, 20)]
        return carry

    lax.fori_loop(0, half // 20, add_core, 0)

    n1, n2 = half // 8, half // 32
    orders = (("y", "x", "z"), ("x", "z", "y"))
    base = [mine + k * (half // 2) for k in range(2)]
    waits = []
    for k, (a1, a2, a3) in enumerate(orders):
        waits.append(
            spread(
                4 + k, a1,
                lambda q, k=k: T.at[pl.ds(base[k] + q * n1, n1)],
                lambda q, k=k: P1.at[k, q],
            )
        )
    first, second = [], []
    for k, (a1, a2, a3) in enumerate(orders):
        me = place[a1]
        P1[k, me] = T[pl.ds(base[k] + me * n1, n1)]
        waits[k]()
        P1[k, 0] = P1[k, 0] + P1[k, 1] + P1[k, 2] + P1[k, 3]
        first.append(
            spread(
                6 + k, a2,
                lambda q, k=k: P1.at[k, 0, pl.ds(q * n2, n2)],
                lambda q, k=k: P2.at[k, q],
            )
        )
    gram_wait()
    G2[x] = G1[0] + G1[1] + G1[2] + G1[3]
    gram_wait = spread(8, "x", lambda k: G2.at[x], lambda k: G2.at[k])
    for k, (a1, a2, a3) in enumerate(orders):
        me = place[a2]
        P2[k, me] = P1[k, 0, pl.ds(me * n2, n2)]
        first[k]()
        m3 = place[a3]
        P3[k, m3] = P2[k, 0] + P2[k, 1] + P2[k, 2] + P2[k, 3]
        second.append(spread(9 + k, a3, lambda q, k=k, m3=m3: P3.at[k, m3], lambda q, k=k: P3.at[k, q]))
    gram_wait()
    gram_out[...] = G2[0] + G2[1] + G2[2] + G2[3]
    third, fourth = [], []
    for k, (a1, a2, a3) in enumerate(orders):
        second[k]()
        row = base[k] + place[a1] * n1
        spot = row + place[a2] * n2
        out[pl.ds(spot, n2)] = P3[k, 0] + P3[k, 1] + P3[k, 2] + P3[k, 3]
        third.append(
            spread(
                11 + k, a2,
                lambda q, spot=spot: out.at[pl.ds(spot, n2)],
                lambda q, row=row: out.at[pl.ds(row + q * n2, n2)],
            )
        )
    for k, (a1, a2, a3) in enumerate(orders):
        third[k]()
        row = base[k] + place[a1] * n1
        fourth.append(
            spread(
                13 + k, a1,
                lambda q, row=row: out.at[pl.ds(row, n1)],
                lambda q, k=k: out.at[pl.ds(base[k] + q * n1, n1)],
            )
        )
    fourth[0]()
    fourth[1]()
    swap(15, out.at[pl.ds(mine, half)], out.at[pl.ds(mine, half)])
    remote(out.at[pl.ds(theirs, half)], out.at[pl.ds(theirs, half)], send.at[15, 0], recv.at[15, 0], mate).wait_recv()
    for copy in pending:
        copy.wait_send()


def sums(part, both):
    rank, rows = part.shape
    tiles = both.shape[1] // 128 * (rank // 8)
    half = tiles // 2
    n1, n2 = half // 8, half // 32
    return pl.pallas_call(
        sums_kernel,
        out_shape=(
            jax.ShapeDtypeStruct((tiles, 8, 128), f32),
            jax.ShapeDtypeStruct((rank, rows), f32),
            jax.ShapeDtypeStruct((rank, rank), f32),
        ),
        in_specs=[vspec(), vspec()],
        out_specs=(vspec(), vspec(), vspec()),
        scratch_shapes=[
            VMEM((rank, rows), f32),
            VMEM((4, rank, rows), f32),
            VMEM((tiles, 8, 128), f32),
            VMEM((half, 8, 128), f32),
            VMEM((2, 4, n1, 8, 128), f32),
            VMEM((2, 4, n2, 8, 128), f32),
            VMEM((2, 4, n2, 8, 128), f32),
            VMEM((4, rank, rank), f32),
            VMEM((4, rank, rank), f32),
            DMA((16, 4)),
            DMA((16, 4)),
        ],
        compiler_params=pltpu.CompilerParams(collective_id=1, has_side_effects=True),
        name="sums",
    )(part, both)


def finish_kernel(coef, total, linv, left_t, both, weight, new_weight, new_mom, new_right, RT, O2, N):
    step = pl.program_id(0)

    @pl.when(step == 0)
    def _():
        sq = jnp.zeros((RT.shape[0], 128), f32)

        def col(j, sq):
            v = jnp.dot(linv[...], total[j], precision=HI, preferred_element_type=f32) * (1.0 / 8.0)
            RT[:, pl.ds(pl.multiple_of(j * 128, 128), 128)] = v
            return sq + v * v

        sq = lax.fori_loop(0, total.shape[0], col, sq)
        norm = lax.rsqrt(jnp.sum(sq, axis=1, keepdims=True) + EPS)
        N[...] = jnp.broadcast_to(norm, N.shape)
        ortho_t = jnp.dot(linv[...], left_t[...], precision=HI, preferred_element_type=f32)
        rows = ortho_t.shape[1]
        O2[0:rows, :] = (ortho_t * (1.0 - MU)).T
        O2[rows : 2 * rows, :] = (ortho_t * norm * coef).T

    rows = both.shape[0]
    rt = RT[:, pl.ds(pl.multiple_of(step * 640, 640), 640)]
    low = jnp.dot(O2[...], rt, precision=HI, preferred_element_type=f32)
    new_mom[...] = both[...] - low[0:rows]
    new_weight[...] = (weight[...].astype(f32) - low[rows:]).astype(bf16)
    new_right[...] = (rt * N[:, 0:1]).T


def finish(coef, total, linv, left_t, both, weight):
    rows, cols = both.shape
    rank = linv.shape[0]
    whole = lambda *shape: pl.BlockSpec(shape, lambda i: (0,) * len(shape))
    blocked = pl.BlockSpec((rows, 640), lambda i: (0, i))
    return pl.pallas_call(
        functools.partial(finish_kernel, coef),
        grid=(cols // 640,),
        out_shape=(
            jax.ShapeDtypeStruct((rows, cols), bf16),
            jax.ShapeDtypeStruct((rows, cols), f32),
            jax.ShapeDtypeStruct((cols, rank), f32),
        ),
        in_specs=[whole(*total.shape), whole(rank, rank), whole(rank, rows), blocked, blocked],
        out_specs=(blocked, blocked, pl.BlockSpec((640, rank), lambda i: (i, 0))),
        scratch_shapes=[VMEM((rank, cols), f32), VMEM((2 * rows, rank), f32), VMEM((rank, 128), f32)],
        name="finish",
    )(total, linv, left_t, both, weight)


def per_device(inputs, cotangent, lengths, momentum, weight, right_factor):
    block_len = inputs.shape[0] // lengths.shape[0]
    position = jnp.arange(block_len, dtype=jnp.int32)
    keep = (position[None, :] < lengths[:, None]).reshape(-1).astype(bf16)
    masked = inputs * keep[:, None]
    half = masked.shape[0] // 2
    packed = jnp.concatenate([masked[:half], masked[half:]], axis=1)
    inv = 1.0 / jnp.sum(lengths.astype(f32))
    both, part = gradient(cotangent, packed, inv.reshape(1), momentum[0], right_factor)
    total, left_t, gram = sums(part, both)
    factor = jnp.linalg.cholesky(gram)
    linv = jax.scipy.linalg.solve_triangular(factor, jnp.eye(gram.shape[0], dtype=f32), lower=True)
    rank = gram.shape[0]
    rows_all = both.shape[0] * lax.axis_size("tensor")
    coef = LR * math.sqrt(rows_all / both.shape[1])
    new_weight, new_mom, new_right = finish(
        coef, total.reshape(-1, rank, 128), linv, left_t, both, weight
    )
    return (new_weight, new_mom[None], new_right)


def solution(mesh):
    placed = (
        P("dp", "tensor"),
        P("dp", "tensor"),
        P("dp"),
        P("dp", "tensor", None),
        P("tensor", None),
        P(),
    )
    return jax.shard_map(
        per_device,
        mesh=mesh,
        in_specs=placed,
        out_specs=(P("tensor", None), P("dp", "tensor", None), P()),
        check_vma=False,
    )
```

```python
import functools
import math

import jax
import jax.numpy as jnp
from jax import lax
from jax.experimental import pallas as pl
from jax.experimental.pallas import tpu as pltpu
from jax.sharding import PartitionSpec as P

EPS = 1e-06
MU = 0.95
LR = 0.02

f32 = jnp.float32
bf16 = jnp.bfloat16
HI = lax.Precision.HIGHEST
VMEM = pltpu.VMEM
DMA = pltpu.SemaphoreType.DMA
CODES = 32767.0
DEPTH = 768


def vspec():
    return pl.BlockSpec(memory_space=pltpu.VMEM)


def anyspec():
    return pl.BlockSpec(memory_space=pl.ANY)


def sspec():
    return pl.BlockSpec(memory_space=pltpu.SMEM)


def around(i, by):
    return lax.rem(i + by, 4)


def cols_of(start, size):
    return pl.ds(pl.multiple_of(start, 128), size)


def split(v):
    high = v.astype(bf16)
    return high, (v - high.astype(f32)).astype(bf16)


def dot(a, b, contract=((1,), (0,))):
    return lax.dot_general(a, b, (contract, ((), ())), preferred_element_type=f32)


def remote(src, dst, send, recv, where):
    return pltpu.make_async_remote_copy(
        src_ref=src,
        dst_ref=dst,
        send_sem=send,
        recv_sem=recv,
        device_id=where,
        device_id_type=pl.DeviceIdType.MESH,
    )


def greet(peers):
    barrier = pltpu.get_barrier_semaphore()
    for peer in peers:
        pl.semaphore_signal(barrier, inc=1, device_id=peer, device_id_type=pl.DeviceIdType.MESH)
    pl.semaphore_wait(barrier, len(peers))


def comm_kernel(
    cot, bt, lengths, mom, rft, both_out, out, linv_out, left_out,
    A, B, codes, scales, R, RS, relay, relay_s, acc, keep, S, R2, both, rfv,
    LT, L0, L1, LL, T, D, P1, P2, P3, G1, G2, M,
    sl, sa, ra, sb, rb, sc, ss, rc, rs, sf, sfs, rf, rfs, send, recv,
):
    t = lax.axis_index("tensor")
    d = lax.axis_index("dp")
    x, z = lax.div(t, 4), lax.rem(t, 4)
    y, c = lax.div(d, 2), lax.rem(d, 2)
    place = {"x": x, "y": y, "z": z}

    def along(axis, k):
        if axis == "core":
            return {"dp": y * 2 + k}
        if axis == "y":
            return {"dp": k * 2 + c}
        if axis == "x":
            return {"tensor": k * 4 + z}
        return {"tensor": x * 4 + k}

    zl, zr, zo = around(z, 3), around(z, 1), around(z, 2)
    xl, xr, xo = around(x, 3), around(x, 1), around(x, 2)
    tok, rows = cot.shape
    feats = bt.shape[0]
    ha, hb = tok // 2, feats // 2
    mate = along("core", 1 - c)

    locals_ = [
        pltpu.make_async_copy(cot, A.at[z], sl.at[0]),
        pltpu.make_async_copy(bt, B.at[x], sl.at[1]),
        pltpu.make_async_copy(mom, both, sl.at[2]),
        pltpu.make_async_copy(rft, rfv, sl.at[3]),
    ]
    greet([mate] + [along(a, around(place[a], q)) for a in "xyz" for q in (1, 2, 3)])

    def part_a(h):
        return pl.ds(h * ha, ha)

    def part_b(h):
        return pl.ds(h * hb, hb)

    sent = []
    for half, right in ((0, True), (1, False), (1, True), (0, False)):
        k = half + (0 if right else 2)
        ca = remote(cot.at[part_a(half)], A.at[z, part_a(half)], sa.at[k], ra.at[k], along("z", zr if right else zl))
        ca.start()
        cb = remote(bt.at[part_b(half)], B.at[x, part_b(half)], sb.at[k], rb.at[k], along("x", xr if right else xl))
        cb.start()
        sent += [ca, cb]
    for copy in locals_:
        copy.start()

    def got_a(k):
        remote(A.at[z, part_a(0)], A.at[z, part_a(0)], sa.at[0], ra.at[k], along("z", zr)).wait_recv()

    def got_b(k):
        remote(B.at[x, part_b(0)], B.at[x, part_b(0)], sb.at[0], rb.at[k], along("x", xr)).wait_recv()

    def pass_a(k, half, origin, to):
        copy = remote(A.at[origin, part_a(half)], A.at[origin, part_a(half)], sa.at[k], ra.at[k], along("z", to))
        copy.start()
        sent.append(copy)

    def pass_b(k, half, origin, to):
        copy = remote(B.at[origin, part_b(half)], B.at[origin, part_b(half)], sb.at[k], rb.at[k], along("x", to))
        copy.start()
        sent.append(copy)

    block_len = tok // lengths.shape[0]
    count = lengths[0]
    for b in range(lengths.shape[0]):
        keep[:, b * block_len : (b + 1) * block_len] = (
            lax.broadcasted_iota(jnp.int32, (16, block_len), 1) < lengths[b]
        ).astype(f32).astype(bf16)
        if b:
            count = count + lengths[b]
    share = 1.0 / jnp.full((1, rows), count, jnp.int32).astype(f32)

    def unit(xx, zz, code_ref, scale_ref):
        acc[...] = jnp.zeros_like(acc)

        def step(k, carry):
            r = cols_of(k * DEPTH, DEPTH)
            acc[...] += dot(B[xx, :, r] * keep[0:1, r], A[zz, r, :])
            return carry

        lax.fori_loop(0, tok // DEPTH, step, 0)
        v = acc[...] * share
        top = jnp.max(jnp.abs(v), axis=0, keepdims=True)
        live = top > 1e-30
        code = jnp.round(v * jnp.where(live, CODES / jnp.where(live, top, 1.0), 0.0))
        code_ref[...] = code.astype(jnp.int32).astype(jnp.int16)
        scale_ref[...] = jnp.broadcast_to(jnp.where(live, top, 0.0) * (1.0 / CODES), (8, rows))

    def made(xx, zz):
        unit(xx, zz, codes.at[xx, zz], scales.at[xx, zz])

    def home(xx, zz):
        remote(codes.at[xx, zz], R.at[xx, z], sc.at[xx, zz], rc.at[xx, z], along("z", zz)).start()
        remote(scales.at[xx, zz], RS.at[xx, z], ss.at[xx, zz], rs.at[xx, z], along("z", zz)).start()

    def half_way(xx, side, n):
        to = along("z", around(z, jnp.where(side == 0, 1, 3)))
        remote(codes.at[xx, zo], relay.at[side, n], sc.at[xx, zo], rf.at[side, n], to).start()
        remote(scales.at[xx, zo], relay_s.at[side, n], ss.at[xx, zo], rfs.at[side, n], to).start()

    def hand_on(o, wait_only=False):
        side, n = o % 2, o // 2
        xx = (x, xl, xr, xo)[o]
        origin, to = (zl, zr) if side == 0 else (zr, zl)
        one = remote(relay.at[side, n], R.at[xx, origin], sf.at[side, n], rf.at[side, n], along("z", to))
        one.wait_recv()
        two = remote(relay_s.at[side, n], RS.at[xx, origin], sfs.at[side, n], rfs.at[side, n], along("z", to))
        two.wait_recv()
        remote(relay.at[side, n], R.at[xx, origin], sf.at[side, n], rc.at[xx, origin], along("z", to)).start()
        remote(relay_s.at[side, n], RS.at[xx, origin], sfs.at[side, n], rs.at[xx, origin], along("z", to)).start()

    locals_[0].wait()
    locals_[1].wait()
    unit(x, z, R.at[x, z], RS.at[x, z])
    locals_[2].wait()
    locals_[3].wait()
    rank = rft.shape[0]
    r_high, r_low = split(rfv[...])
    R2[0:rank] = r_high
    R2[rank : 2 * rank] = r_low
    LT[...] = jnp.zeros_like(LT)

    def mom_left(g, carry):
        r = cols_of(g * 256, 256)
        high, low = split(both[:, r])
        v = dot(R2[:, r], high, ((1,), (1,)))
        LT[...] += v[0:rank] + v[rank:] + dot(R2[0:rank, r], low, ((1,), (1,)))
        return carry

    lax.fori_loop(0, both.shape[1] // 256, mom_left, 0)

    got_a(0)
    pass_a(4, 0, zl, zr)
    got_a(3)
    pass_a(5, 1, zr, zl)
    got_b(0)
    pass_b(4, 0, xl, xr)
    got_b(3)
    pass_b(5, 1, xr, xl)
    got_a(1)
    got_a(2)

    def own_cols(i, carry):
        zz = around(z, 3 - 2 * i)
        made(x, zz)
        home(x, zz)
        return carry

    lax.fori_loop(0, 2, own_cols, 0)
    got_b(1)
    got_b(2)

    def next_cols(i, carry):
        xx = around(x, 3 - 2 * lax.div(i, 3))
        m = lax.rem(i, 3)

        @pl.when(m == 2)
        def _():
            unit(xx, z, R.at[xx, z], RS.at[xx, z])

        @pl.when(m != 2)
        def _():
            made(xx, around(z, 3 - 2 * m))

        return carry

    lax.fori_loop(0, 6, next_cols, 0)
    got_a(4)
    got_a(5)

    def far_rows(i, carry):
        xx = around(x, jnp.where(i == 0, 0, 5 - 2 * i))
        made(xx, zo)
        half_way(xx, lax.rem(i, 2), lax.div(i, 2))
        return carry

    lax.fori_loop(0, 3, far_rows, 0)
    for xx in (xl, xr):
        home(xx, zl)
        home(xx, zr)
    for o in range(3):
        hand_on(o)
    got_b(4)
    got_b(5)

    def far_cols(i, carry):
        @pl.when(i == 0)
        def _():
            made(xo, zo)
            half_way(xo, 1, 1)

        @pl.when(jnp.logical_and(i != 0, i != 3))
        def _():
            zz = around(z, 5 - 2 * i)
            made(xo, zz)
            home(xo, zz)

        @pl.when(i == 3)
        def _():
            unit(xo, z, R.at[xo, z], RS.at[xo, z])

        return carry

    lax.fori_loop(0, 4, far_cols, 0)
    hand_on(3)

    def gather_home(o, carry):
        xx = around(x, jnp.where(o == 0, 0, jnp.where(o == 3, 2, 5 - 2 * o)))
        for by in (1, 3, 2):
            zz = around(z, by)
            remote(codes.at[0, 0], R.at[xx, zz], sc.at[0, 0], rc.at[xx, zz], along("z", zz)).wait_recv()
            remote(scales.at[0, 0], RS.at[xx, zz], ss.at[0, 0], rs.at[xx, zz], along("z", zz)).wait_recv()
        for h in range(2):
            base = xx * (4 * feats) + h * (2 * feats)
            for i in range(2):
                S[i * feats : (i + 1) * feats] = R[xx, 2 * h + i].astype(jnp.int32).astype(f32) * RS[xx, 2 * h + i, 0:1]
            high, low = split(S[...])
            r = cols_of(base, 2 * feats)
            v = dot(R2[:, r], high)
            LT[...] += v[0:rank] + v[rank:] + dot(R2[0:rank, r], low)
            for i in range(2 * feats // 128):
                both[:, cols_of(base + 128 * i, 128)] += S[128 * i : 128 * (i + 1)].T
        return carry

    lax.fori_loop(0, 4, gather_home, 0)

    save = pltpu.make_async_copy(both, both_out, sl.at[4])
    save.start()
    pending = []

    def swap(stage, src, dst):
        copy = remote(src, dst, send.at[stage, 0], recv.at[stage, 0], mate)
        copy.start()
        pending.append(copy)
        return copy

    def spread(stage, axis, src, dst):
        me = place[axis]
        waits = []
        for q in (2, 1, 3):
            k = around(me, q)
            copy = remote(src(k), dst(me), send.at[stage, q], recv.at[stage, q], along(axis, k))
            copy.start()
            pending.append(copy)
            waits.append(remote(src(k), dst(around(me, 4 - q)), send.at[stage, q], recv.at[stage, q], along(axis, k)))

        def wait():
            for w in waits:
                w.wait_recv()

        return wait

    swap(0, LT, L0).wait_recv()
    L1[y] = LT[...] + L0[...]
    spread(1, "y", lambda k: L1.at[y], lambda k: L1.at[k])()
    left = (L1[0] + L1[1] + L1[2] + L1[3]) * (1.0 / 8.0)
    left_out[...] = left
    left_high, left_low = split(left)
    LL[0:rank] = left_high
    LL[rank : 2 * rank] = left_low
    v = dot(LL[...], left_high, ((1,), (1,)))
    G1[z] = v[0:rank] + v[rank:] + dot(left_high, left_low, ((1,), (1,)))
    gram_wait = spread(2, "z", lambda k: G1.at[z], lambda k: G1.at[k])

    tiles = both.shape[1] // 128 * (rank // 8)
    half = tiles // 2
    blocks = both.shape[1] // 512

    def block(g, carry):
        high, low = split(both[:, cols_of(g * 256, 256)])
        v = dot(LL[...], high)
        v = v[0:rank] + v[rank:] + dot(LL[0:rank], low)
        for i in range(2):
            T[pl.ds(g * 16 + i * 8, 8)] = v[:, 128 * i : 128 * (i + 1)].reshape(8, 8, 128)
        return carry

    lax.fori_loop(blocks * (1 - c), blocks * (2 - c), block, 0)
    mine, theirs = c * half, (1 - c) * half
    core_wait = swap(3, T.at[pl.ds(theirs, half)], D)
    lax.fori_loop(blocks * c, blocks * (1 + c), block, 0)
    core_wait.wait_recv()

    def add_core(g, carry):
        r = pl.ds(mine + g * 20, 20)
        T[r] = T[r] + D[pl.ds(g * 20, 20)]
        return carry

    lax.fori_loop(0, half // 20, add_core, 0)

    n1, n2 = half // 8, half // 32
    orders = (("y", "x", "z"), ("x", "z", "y"))
    base = [mine + k * (half // 2) for k in range(2)]
    zeroth, first, second, third, fourth = [], [], [], [], []
    for k, (a1, a2, a3) in enumerate(orders):
        zeroth.append(
            spread(
                4 + k, a1,
                lambda q, k=k: T.at[pl.ds(base[k] + q * n1, n1)],
                lambda q, k=k: P1.at[k, q],
            )
        )
    gram_wait()
    G2[x] = G1[0] + G1[1] + G1[2] + G1[3]
    gram_wait = spread(8, "x", lambda k: G2.at[x], lambda k: G2.at[k])
    for k, (a1, a2, a3) in enumerate(orders):
        me = place[a1]
        P1[k, me] = T[pl.ds(base[k] + me * n1, n1)]
        zeroth[k]()
        P1[k, 0] = P1[k, 0] + P1[k, 1] + P1[k, 2] + P1[k, 3]
        first.append(
            spread(
                6 + k, a2,
                lambda q, k=k: P1.at[k, 0, pl.ds(q * n2, n2)],
                lambda q, k=k: P2.at[k, q],
            )
        )
    row_id = lax.broadcasted_iota(jnp.int32, (rank, 2 * rank), 0)
    lane_id = lax.broadcasted_iota(jnp.int32, (rank, 2 * rank), 1)
    gram_wait()
    M[...] = jnp.where(lane_id == row_id + rank, 1.0, 0.0)
    M[:, 0:rank] = G2[0] + G2[1] + G2[2] + G2[3]

    def pivot(k, carry):
        m = M[...]
        row = M[pl.ds(k, 1), :]
        top = jnp.sum(jnp.where(lane_id[0:1] == k, row, 0.0), axis=1, keepdims=True)
        factor = jnp.sum(jnp.where(lane_id == k, m, 0.0), axis=1, keepdims=True)
        factor = jnp.where(row_id[:, 0:1] > k, factor / top, 0.0)
        M[...] = m - factor * row
        return carry

    cuts = (0, 16, 32, 48, rank)
    lax.fori_loop(cuts[0], cuts[1], pivot, 0)
    for k, (a1, a2, a3) in enumerate(orders):
        me = place[a2]
        P2[k, me] = P1[k, 0, pl.ds(me * n2, n2)]
        first[k]()
        m3 = place[a3]
        P3[k, m3] = P2[k, 0] + P2[k, 1] + P2[k, 2] + P2[k, 3]
        second.append(spread(9 + k, a3, lambda q, k=k, m3=m3: P3.at[k, m3], lambda q, k=k: P3.at[k, q]))
    lax.fori_loop(cuts[1], cuts[2], pivot, 0)
    for k, (a1, a2, a3) in enumerate(orders):
        second[k]()
        row = base[k] + place[a1] * n1
        spot = row + place[a2] * n2
        out[pl.ds(spot, n2)] = P3[k, 0] + P3[k, 1] + P3[k, 2] + P3[k, 3]
        third.append(
            spread(
                11 + k, a2,
                lambda q, spot=spot: out.at[pl.ds(spot, n2)],
                lambda q, row=row: out.at[pl.ds(row + q * n2, n2)],
            )
        )
    lax.fori_loop(cuts[2], cuts[3], pivot, 0)
    for k, (a1, a2, a3) in enumerate(orders):
        third[k]()
        row = base[k] + place[a1] * n1
        fourth.append(
            spread(
                13 + k, a1,
                lambda q, row=row: out.at[pl.ds(row, n1)],
                lambda q, k=k: out.at[pl.ds(base[k] + q * n1, n1)],
            )
        )
    lax.fori_loop(cuts[3], cuts[4], pivot, 0)
    m = M[...]
    diag = jnp.sum(jnp.where(lane_id == row_id, m, 0.0), axis=1, keepdims=True)
    linv_out[...] = pltpu.roll(m / jnp.sqrt(diag), rank, 1)[:, 0:rank]
    fourth[0]()
    fourth[1]()
    swap(15, out.at[pl.ds(mine, half)], out.at[pl.ds(mine, half)])
    remote(out.at[pl.ds(theirs, half)], out.at[pl.ds(theirs, half)], send.at[15, 0], recv.at[15, 0], mate).wait_recv()

    for copy in pending + sent:
        copy.wait_send()
    for by in (1, 2, 3):
        for xx in range(4):
            zz = around(z, by)
            remote(codes.at[xx, zz], R.at[0, 0], sc.at[xx, zz], rc.at[0, 0], along("z", zr)).wait_send()
            remote(scales.at[xx, zz], RS.at[0, 0], ss.at[xx, zz], rs.at[0, 0], along("z", zr)).wait_send()
    for o in range(4):
        side, n = o % 2, o // 2
        remote(relay.at[side, n], R.at[0, 0], sf.at[side, n], rc.at[0, 0], along("z", zr)).wait_send()
        remote(relay_s.at[side, n], RS.at[0, 0], sfs.at[side, n], rs.at[0, 0], along("z", zr)).wait_send()
    save.wait()


def communicate(cot, bt, lengths, mom, rft):
    tok, rows = cot.shape
    feats = bt.shape[0]
    rank, cols = rft.shape
    tiles = cols // 128 * (rank // 8)
    half = tiles // 2
    n1, n2 = half // 8, half // 32
    return pl.pallas_call(
        comm_kernel,
        out_shape=(
            jax.ShapeDtypeStruct((rows, cols), f32),
            jax.ShapeDtypeStruct((tiles, 8, 128), f32),
            jax.ShapeDtypeStruct((rank, rank), f32),
            jax.ShapeDtypeStruct((rank, rows), f32),
        ),
        in_specs=[anyspec(), anyspec(), sspec(), anyspec(), anyspec()],
        out_specs=(anyspec(), vspec(), vspec(), vspec()),
        scratch_shapes=[
            VMEM((4, tok, rows), bf16),
            VMEM((4, feats, tok), bf16),
            VMEM((4, 4, feats, rows), jnp.int16),
            VMEM((4, 4, 8, rows), f32),
            VMEM((4, 4, feats, rows), jnp.int16),
            VMEM((4, 4, 8, rows), f32),
            VMEM((2, 2, feats, rows), jnp.int16),
            VMEM((2, 2, 8, rows), f32),
            VMEM((feats, rows), f32),
            VMEM((16, tok), bf16),
            VMEM((2 * feats, rows), f32),
            VMEM((2 * rank, cols), bf16),
            VMEM((rows, cols), f32),
            VMEM((rank, cols), f32),
            VMEM((rank, rows), f32),
            VMEM((rank, rows), f32),
            VMEM((4, rank, rows), f32),
            VMEM((2 * rank, rows), bf16),
            VMEM((tiles, 8, 128), f32),
            VMEM((half, 8, 128), f32),
            VMEM((2, 4, n1, 8, 128), f32),
            VMEM((2, 4, n2, 8, 128), f32),
            VMEM((2, 4, n2, 8, 128), f32),
            VMEM((4, rank, rank), f32),
            VMEM((4, rank, rank), f32),
            VMEM((rank, 2 * rank), f32),
            DMA((5,)), DMA((6,)), DMA((6,)), DMA((6,)), DMA((6,)),
            DMA((4, 4)), DMA((4, 4)), DMA((4, 4)), DMA((4, 4)),
            DMA((2, 2)), DMA((2, 2)), DMA((2, 2)), DMA((2, 2)),
            DMA((16, 4)), DMA((16, 4)),
        ],
        compiler_params=pltpu.CompilerParams(collective_id=0, has_side_effects=True),
        name="communicate",
    )(cot, bt, lengths, mom, rft)


def finish_kernel(
    coef, total, linv, left_t, both, weight, new_weight, new_mom, new_right_t,
    bv, wv, RT, R3, O3, NR, isem, osem,
):
    rows, cols = both.shape
    rank = linv.shape[0]
    wide = cols // 8

    def fetch(i):
        r = cols_of(i * wide, wide)
        return (
            pltpu.make_async_copy(both.at[:, r], bv.at[:, r], isem.at[i, 0]),
            pltpu.make_async_copy(weight.at[:, r], wv.at[:, r], isem.at[i, 1]),
        )

    def store(i):
        r = cols_of(i * wide, wide)
        return (
            pltpu.make_async_copy(bv.at[:, r], new_mom.at[:, r], osem.at[i, 0]),
            pltpu.make_async_copy(wv.at[:, r], new_weight.at[:, r], osem.at[i, 1]),
        )

    for i in range(8):
        for copy in fetch(i):
            copy.start()
    l_high, l_low = split(linv[...] * (1.0 / 8.0))

    def col(j, sq):
        high, low = split(jnp.concatenate([total[2 * j], total[2 * j + 1]], axis=1))
        v = dot(l_high, high) + dot(l_low, high) + dot(l_high, low)
        r = cols_of(j * 256, 256)
        RT[:, r] = v
        v_high, v_low = split(v)
        R3[0:rank, r] = v_high
        R3[rank : 2 * rank, r] = v_low
        R3[2 * rank : 3 * rank, r] = v_high
        return sq + v * v

    sq = lax.fori_loop(0, cols // 256, col, jnp.zeros((rank, 256), f32))
    norm = lax.rsqrt(jnp.sum(sq, axis=1, keepdims=True) + EPS)
    NR[...] = RT[...] * norm
    tell = pltpu.make_async_copy(NR, new_right_t, osem.at[8, 0])
    tell.start()
    ortho_t = jnp.dot(linv[...], left_t[...], precision=HI, preferred_element_type=f32)
    both_t = jnp.concatenate([ortho_t * (1.0 - MU), ortho_t * (norm * coef)], axis=1)
    o_high, o_low = split(both_t)
    O3[...] = jnp.concatenate([o_high, o_high, o_low], axis=0).T

    def work(i, carry):
        for copy in fetch(i):
            copy.wait()
        r = cols_of(i * wide, wide)
        low = dot(O3[...], R3[:, r])
        bv[:, r] = bv[:, r] - low[0:rows]
        wv[:, r] = (wv[:, r].astype(f32) - low[rows:]).astype(bf16)
        for copy in store(i):
            copy.start()
        return carry

    lax.fori_loop(0, 8, work, 0)
    for i in range(8):
        for copy in store(i):
            copy.wait()
    tell.wait()


def finish(coef, total, linv, left_t, both, weight):
    rows, cols = both.shape
    rank = linv.shape[0]
    return pl.pallas_call(
        functools.partial(finish_kernel, coef),
        out_shape=(
            jax.ShapeDtypeStruct((rows, cols), bf16),
            jax.ShapeDtypeStruct((rows, cols), f32),
            jax.ShapeDtypeStruct((rank, cols), f32),
        ),
        in_specs=[vspec(), vspec(), vspec(), anyspec(), anyspec()],
        out_specs=(anyspec(), anyspec(), anyspec()),
        scratch_shapes=[
            VMEM((rows, cols), f32),
            VMEM((rows, cols), bf16),
            VMEM((rank, cols), f32),
            VMEM((3 * rank, cols), bf16),
            VMEM((2 * rows, 3 * rank), bf16),
            VMEM((rank, cols), f32),
            DMA((8, 2)),
            DMA((9, 2)),
        ],
        name="finish",
    )(total, linv, left_t, both, weight)


def per_device(inputs, cotangent, lengths, momentum, weight, right_factor):
    both, total, linv, left_t = communicate(cotangent, inputs.T, lengths, momentum[0], right_factor.T)
    rank = linv.shape[0]
    rows_all = both.shape[0] * lax.axis_size("tensor")
    coef = LR * math.sqrt(rows_all / both.shape[1])
    new_weight, new_mom, new_right_t = finish(
        coef, total.reshape(-1, rank, 128), linv, left_t, both, weight
    )
    return (new_weight, new_mom[None], new_right_t.T)


def solution(mesh):
    placed = (
        P("dp", "tensor"),
        P("dp", "tensor"),
        P("dp"),
        P("dp", "tensor", None),
        P("tensor", None),
        P(),
    )
    return jax.shard_map(
        per_device,
        mesh=mesh,
        in_specs=placed,
        out_specs=(P("tensor", None), P("dp", "tensor", None), P()),
        check_vma=False,
    )
```

```python
import functools
import math

import jax
import jax.numpy as jnp
from jax import lax
from jax.experimental import pallas as pl
from jax.experimental.pallas import tpu as pltpu
from jax.sharding import PartitionSpec as P

EPS = 1e-06
MU = 0.95
LR = 0.02

f32 = jnp.float32
bf16 = jnp.bfloat16
HI = lax.Precision.HIGHEST
VMEM = pltpu.VMEM
DMA = pltpu.SemaphoreType.DMA
CODES = 32767.0
DEPTH = 768


def vspec():
    return pl.BlockSpec(memory_space=pltpu.VMEM)


def anyspec():
    return pl.BlockSpec(memory_space=pl.ANY)


def sspec():
    return pl.BlockSpec(memory_space=pltpu.SMEM)


def around(i, by):
    return lax.rem(i + by, 4)


def cols_of(start, size):
    return pl.ds(pl.multiple_of(start, 128), size)


def split(v):
    high = v.astype(bf16)
    return high, (v - high.astype(f32)).astype(bf16)


def dot(a, b, contract=((1,), (0,))):
    return lax.dot_general(a, b, (contract, ((), ())), preferred_element_type=f32)


def remote(src, dst, send, recv, where):
    return pltpu.make_async_remote_copy(
        src_ref=src,
        dst_ref=dst,
        send_sem=send,
        recv_sem=recv,
        device_id=where,
        device_id_type=pl.DeviceIdType.MESH,
    )


def greet(peers):
    barrier = pltpu.get_barrier_semaphore()
    for peer in peers:
        pl.semaphore_signal(barrier, inc=1, device_id=peer, device_id_type=pl.DeviceIdType.MESH)
    pl.semaphore_wait(barrier, len(peers))


def comm_kernel(
    cot, bt, lengths, mom, rft, both_out, out, linv_out, left_out,
    A, B, codes, scales, R, RS, relay, relay_s, acc, keep, S, R2, both, rfv,
    LT, L0, L1, LL, T, D, P1, P2, P3, G1, G2, M,
    sl, sa, ra, sb, rb, sc, ss, rc, rs, sf, sfs, rf, rfs, send, recv,
):
    t = lax.axis_index("tensor")
    d = lax.axis_index("dp")
    x, z = lax.div(t, 4), lax.rem(t, 4)
    y, c = lax.div(d, 2), lax.rem(d, 2)
    place = {"x": x, "y": y, "z": z}

    def along(axis, k):
        if axis == "core":
            return {"dp": y * 2 + k}
        if axis == "y":
            return {"dp": k * 2 + c}
        if axis == "x":
            return {"tensor": k * 4 + z}
        if axis == "z":
            return {"tensor": x * 4 + k}
        if axis == "a":
            return {"tensor": (1 - c) * (x * 4 + k) + c * (k * 4 + z)}
        return {"tensor": (1 - c) * (k * 4 + z) + c * (x * 4 + k)}

    pa = (1 - c) * z + c * x
    pb = (1 - c) * x + c * z
    al, ar, ao = around(pa, 3), around(pa, 1), around(pa, 2)
    bl, br, bo = around(pb, 3), around(pb, 1), around(pb, 2)
    tok, rows = cot.shape
    feats = bt.shape[0]
    ha, hb = tok // 2, feats // 2
    mate = along("core", 1 - c)

    locals_ = [
        pltpu.make_async_copy(cot, A.at[pa], sl.at[0]),
        pltpu.make_async_copy(bt, B.at[pb], sl.at[1]),
        pltpu.make_async_copy(mom, both, sl.at[2]),
        pltpu.make_async_copy(rft, rfv, sl.at[3]),
    ]
    greet([mate] + [along(a, around(place[a], q)) for a in "xyz" for q in (1, 2, 3)])

    def part_a(h):
        return pl.ds(h * ha, ha)

    def part_b(h):
        return pl.ds(h * hb, hb)

    sent = []
    for half, right in ((0, True), (1, False), (1, True), (0, False)):
        k = half + (0 if right else 2)
        ca = remote(cot.at[part_a(half)], A.at[pa, part_a(half)], sa.at[k], ra.at[k], along("a", ar if right else al))
        ca.start()
        cb = remote(bt.at[part_b(half)], B.at[pb, part_b(half)], sb.at[k], rb.at[k], along("b", br if right else bl))
        cb.start()
        sent += [ca, cb]
    for copy in locals_:
        copy.start()

    def got_a(k):
        remote(A.at[pa, part_a(0)], A.at[pa, part_a(0)], sa.at[0], ra.at[k], along("a", ar)).wait_recv()

    def got_b(k):
        remote(B.at[pb, part_b(0)], B.at[pb, part_b(0)], sb.at[0], rb.at[k], along("b", br)).wait_recv()

    def pass_a(k, half, origin, to):
        copy = remote(A.at[origin, part_a(half)], A.at[origin, part_a(half)], sa.at[k], ra.at[k], along("a", to))
        copy.start()
        sent.append(copy)

    def pass_b(k, half, origin, to):
        copy = remote(B.at[origin, part_b(half)], B.at[origin, part_b(half)], sb.at[k], rb.at[k], along("b", to))
        copy.start()
        sent.append(copy)

    block_len = tok // lengths.shape[0]
    count = lengths[0]
    for b in range(lengths.shape[0]):
        keep[:, b * block_len : (b + 1) * block_len] = (
            lax.broadcasted_iota(jnp.int32, (16, block_len), 1) < lengths[b]
        ).astype(f32).astype(bf16)
        if b:
            count = count + lengths[b]
    share = 1.0 / jnp.full((1, rows), count, jnp.int32).astype(f32)

    def unit(xx, zz, code_ref, scale_ref):
        acc[...] = jnp.zeros_like(acc)

        def step(k, carry):
            r = cols_of(k * DEPTH, DEPTH)
            acc[...] += dot(B[xx, :, r] * keep[0:1, r], A[zz, r, :])
            return carry

        lax.fori_loop(0, tok // DEPTH, step, 0)
        v = acc[...] * share
        top = jnp.max(jnp.abs(v), axis=0, keepdims=True)
        live = top > 1e-30
        code = jnp.round(v * jnp.where(live, CODES / jnp.where(live, top, 1.0), 0.0))
        code_ref[...] = code.astype(jnp.int32).astype(jnp.int16)
        scale_ref[...] = jnp.broadcast_to(jnp.where(live, top, 0.0) * (1.0 / CODES), (8, rows))

    def made(xx, zz):
        unit(xx, zz, codes.at[xx, zz], scales.at[xx, zz])

    def home(xx, zz):
        remote(codes.at[xx, zz], R.at[xx, pa], sc.at[xx, zz], rc.at[xx, pa], along("a", zz)).start()
        remote(scales.at[xx, zz], RS.at[xx, pa], ss.at[xx, zz], rs.at[xx, pa], along("a", zz)).start()

    def half_way(xx, side, n):
        to = along("a", around(pa, jnp.where(side == 0, 1, 3)))
        remote(codes.at[xx, ao], relay.at[side, n], sc.at[xx, ao], rf.at[side, n], to).start()
        remote(scales.at[xx, ao], relay_s.at[side, n], ss.at[xx, ao], rfs.at[side, n], to).start()

    def hand_on(o, wait_only=False):
        side, n = o % 2, o // 2
        xx = (pb, bl, br, bo)[o]
        origin, to = (al, ar) if side == 0 else (ar, al)
        one = remote(relay.at[side, n], R.at[xx, origin], sf.at[side, n], rf.at[side, n], along("a", to))
        one.wait_recv()
        two = remote(relay_s.at[side, n], RS.at[xx, origin], sfs.at[side, n], rfs.at[side, n], along("a", to))
        two.wait_recv()
        remote(relay.at[side, n], R.at[xx, origin], sf.at[side, n], rc.at[xx, origin], along("a", to)).start()
        remote(relay_s.at[side, n], RS.at[xx, origin], sfs.at[side, n], rs.at[xx, origin], along("a", to)).start()

    locals_[0].wait()
    locals_[1].wait()
    unit(pb, pa, R.at[pb, pa], RS.at[pb, pa])
    locals_[2].wait()
    locals_[3].wait()
    rank = rft.shape[0]
    r_high, r_low = split(rfv[...])
    R2[0:rank] = r_high
    R2[rank : 2 * rank] = r_low
    LT[...] = jnp.zeros_like(LT)

    def mom_left(g, carry):
        r = cols_of(g * 256, 256)
        high, low = split(both[:, r])
        v = dot(R2[:, r], high, ((1,), (1,)))
        LT[...] += v[0:rank] + v[rank:] + dot(R2[0:rank, r], low, ((1,), (1,)))
        return carry

    lax.fori_loop(0, both.shape[1] // 256, mom_left, 0)

    got_a(0)
    pass_a(4, 0, al, ar)
    got_a(3)
    pass_a(5, 1, ar, al)
    got_b(0)
    pass_b(4, 0, bl, br)
    got_b(3)
    pass_b(5, 1, br, bl)
    got_a(1)
    got_a(2)

    def own_cols(i, carry):
        zz = around(pa, 3 - 2 * i)
        made(pb, zz)
        home(pb, zz)
        return carry

    lax.fori_loop(0, 2, own_cols, 0)
    got_b(1)
    got_b(2)

    def next_cols(i, carry):
        xx = around(pb, 3 - 2 * lax.div(i, 3))
        m = lax.rem(i, 3)

        @pl.when(m == 2)
        def _():
            unit(xx, pa, R.at[xx, pa], RS.at[xx, pa])

        @pl.when(m != 2)
        def _():
            made(xx, around(pa, 3 - 2 * m))

        return carry

    lax.fori_loop(0, 6, next_cols, 0)
    got_a(4)
    got_a(5)

    def far_rows(i, carry):
        xx = around(pb, jnp.where(i == 0, 0, 5 - 2 * i))
        made(xx, ao)
        half_way(xx, lax.rem(i, 2), lax.div(i, 2))
        return carry

    lax.fori_loop(0, 3, far_rows, 0)
    for xx in (bl, br):
        home(xx, al)
        home(xx, ar)
    for o in range(3):
        hand_on(o)
    got_b(4)
    got_b(5)

    def far_cols(i, carry):
        @pl.when(i == 0)
        def _():
            made(bo, ao)
            half_way(bo, 1, 1)

        @pl.when(jnp.logical_and(i != 0, i != 3))
        def _():
            zz = around(pa, 5 - 2 * i)
            made(bo, zz)
            home(bo, zz)

        @pl.when(i == 3)
        def _():
            unit(bo, pa, R.at[bo, pa], RS.at[bo, pa])

        return carry

    lax.fori_loop(0, 4, far_cols, 0)
    hand_on(3)

    late = lax.div(bo, 2)

    def gather_home(n, carry):
        o, h = lax.div(n, 2), lax.rem(n, 2)
        xx = around(pb, jnp.where(o == 0, 0, jnp.where(o == 3, 2, 5 - 2 * o)))
        group = jnp.where(n < 4, 1 - late, late)
        base = jnp.where(c == 0, xx * 2 + h, lax.rem(n, 4) * 2 + group) * (2 * feats)
        for i in range(2):
            xi = jnp.where(c == 0, xx, 2 * group + i)
            zi = jnp.where(c == 0, 2 * h + i, lax.rem(n, 4))

            @pl.when(zi != pa)
            def _():
                remote(codes.at[0, 0], R.at[xi, zi], sc.at[0, 0], rc.at[xi, zi], along("a", ar)).wait_recv()
                remote(scales.at[0, 0], RS.at[xi, zi], ss.at[0, 0], rs.at[xi, zi], along("a", ar)).wait_recv()

            S[i * feats : (i + 1) * feats] = R[xi, zi].astype(jnp.int32).astype(f32) * RS[xi, zi, 0:1]
        high, low = split(S[...])
        r = cols_of(base, 2 * feats)
        v = dot(R2[:, r], high)
        LT[...] += v[0:rank] + v[rank:] + dot(R2[0:rank, r], low)
        for i in range(2 * feats // 128):
            both[:, cols_of(base + 128 * i, 128)] += S[128 * i : 128 * (i + 1)].T
        return carry

    lax.fori_loop(0, 8, gather_home, 0)

    save = pltpu.make_async_copy(both, both_out, sl.at[4])
    save.start()
    pending = []

    def swap(stage, src, dst):
        copy = remote(src, dst, send.at[stage, 0], recv.at[stage, 0], mate)
        copy.start()
        pending.append(copy)
        return copy

    def spread(stage, axis, src, dst):
        me = place[axis]
        waits = []
        for q in (2, 1, 3):
            k = around(me, q)
            copy = remote(src(k), dst(me), send.at[stage, q], recv.at[stage, q], along(axis, k))
            copy.start()
            pending.append(copy)
            waits.append(remote(src(k), dst(around(me, 4 - q)), send.at[stage, q], recv.at[stage, q], along(axis, k)))

        def wait():
            for w in waits:
                w.wait_recv()

        return wait

    swap(0, LT, L0).wait_recv()
    L1[y] = LT[...] + L0[...]
    spread(1, "y", lambda k: L1.at[y], lambda k: L1.at[k])()
    left = (L1[0] + L1[1] + L1[2] + L1[3]) * (1.0 / 8.0)
    left_out[...] = left
    left_high, left_low = split(left)
    LL[0:rank] = left_high
    LL[rank : 2 * rank] = left_low
    v = dot(LL[...], left_high, ((1,), (1,)))
    G1[z] = v[0:rank] + v[rank:] + dot(left_high, left_low, ((1,), (1,)))
    gram_wait = spread(2, "z", lambda k: G1.at[z], lambda k: G1.at[k])

    tiles = both.shape[1] // 128 * (rank // 8)
    half = tiles // 2
    blocks = both.shape[1] // 512

    def block(g, carry):
        high, low = split(both[:, cols_of(g * 256, 256)])
        v = dot(LL[...], high)
        v = v[0:rank] + v[rank:] + dot(LL[0:rank], low)
        for i in range(2):
            T[pl.ds(g * 16 + i * 8, 8)] = v[:, 128 * i : 128 * (i + 1)].reshape(8, 8, 128)
        return carry

    lax.fori_loop(blocks * (1 - c), blocks * (2 - c), block, 0)
    mine, theirs = c * half, (1 - c) * half
    core_wait = swap(3, T.at[pl.ds(theirs, half)], D)
    lax.fori_loop(blocks * c, blocks * (1 + c), block, 0)
    core_wait.wait_recv()

    def add_core(g, carry):
        r = pl.ds(mine + g * 20, 20)
        T[r] = T[r] + D[pl.ds(g * 20, 20)]
        return carry

    lax.fori_loop(0, half // 20, add_core, 0)

    n1, n2 = half // 8, half // 32
    orders = (("y", "x", "z"), ("x", "z", "y"))
    base = [mine + k * (half // 2) for k in range(2)]
    zeroth, first, second, third, fourth = [], [], [], [], []
    for k, (a1, a2, a3) in enumerate(orders):
        zeroth.append(
            spread(
                4 + k, a1,
                lambda q, k=k: T.at[pl.ds(base[k] + q * n1, n1)],
                lambda q, k=k: P1.at[k, q],
            )
        )
    gram_wait()
    G2[x] = G1[0] + G1[1] + G1[2] + G1[3]
    gram_wait = spread(8, "x", lambda k: G2.at[x], lambda k: G2.at[k])
    for k, (a1, a2, a3) in enumerate(orders):
        me = place[a1]
        P1[k, me] = T[pl.ds(base[k] + me * n1, n1)]
        zeroth[k]()
        P1[k, 0] = P1[k, 0] + P1[k, 1] + P1[k, 2] + P1[k, 3]
        first.append(
            spread(
                6 + k, a2,
                lambda q, k=k: P1.at[k, 0, pl.ds(q * n2, n2)],
                lambda q, k=k: P2.at[k, q],
            )
        )
    row_id = lax.broadcasted_iota(jnp.int32, (rank, 2 * rank), 0)
    lane_id = lax.broadcasted_iota(jnp.int32, (rank, 2 * rank), 1)
    gram_wait()
    M[...] = jnp.where(lane_id == row_id + rank, 1.0, 0.0)
    M[:, 0:rank] = G2[0] + G2[1] + G2[2] + G2[3]

    def pivot(k, carry):
        m = M[...]
        row = M[pl.ds(k, 1), :]
        top = jnp.sum(jnp.where(lane_id[0:1] == k, row, 0.0), axis=1, keepdims=True)
        factor = jnp.sum(jnp.where(lane_id == k, m, 0.0), axis=1, keepdims=True)
        factor = jnp.where(row_id[:, 0:1] > k, factor / top, 0.0)
        M[...] = m - factor * row
        return carry

    cuts = (0, 16, 32, 48, rank)
    lax.fori_loop(cuts[0], cuts[1], pivot, 0)
    for k, (a1, a2, a3) in enumerate(orders):
        me = place[a2]
        P2[k, me] = P1[k, 0, pl.ds(me * n2, n2)]
        first[k]()
        m3 = place[a3]
        P3[k, m3] = P2[k, 0] + P2[k, 1] + P2[k, 2] + P2[k, 3]
        second.append(spread(9 + k, a3, lambda q, k=k, m3=m3: P3.at[k, m3], lambda q, k=k: P3.at[k, q]))
    lax.fori_loop(cuts[1], cuts[2], pivot, 0)
    for k, (a1, a2, a3) in enumerate(orders):
        second[k]()
        row = base[k] + place[a1] * n1
        spot = row + place[a2] * n2
        out[pl.ds(spot, n2)] = P3[k, 0] + P3[k, 1] + P3[k, 2] + P3[k, 3]
        third.append(
            spread(
                11 + k, a2,
                lambda q, spot=spot: out.at[pl.ds(spot, n2)],
                lambda q, row=row: out.at[pl.ds(row + q * n2, n2)],
            )
        )
    lax.fori_loop(cuts[2], cuts[3], pivot, 0)
    for k, (a1, a2, a3) in enumerate(orders):
        third[k]()
        row = base[k] + place[a1] * n1
        fourth.append(
            spread(
                13 + k, a1,
                lambda q, row=row: out.at[pl.ds(row, n1)],
                lambda q, k=k: out.at[pl.ds(base[k] + q * n1, n1)],
            )
        )
    lax.fori_loop(cuts[3], cuts[4], pivot, 0)
    m = M[...]
    diag = jnp.sum(jnp.where(lane_id == row_id, m, 0.0), axis=1, keepdims=True)
    linv_out[...] = pltpu.roll(m / jnp.sqrt(diag), rank, 1)[:, 0:rank]
    fourth[0]()
    fourth[1]()
    swap(15, out.at[pl.ds(mine, half)], out.at[pl.ds(mine, half)])
    remote(out.at[pl.ds(theirs, half)], out.at[pl.ds(theirs, half)], send.at[15, 0], recv.at[15, 0], mate).wait_recv()

    for copy in pending + sent:
        copy.wait_send()
    for by in (1, 2, 3):
        for xx in range(4):
            zz = around(pa, by)
            remote(codes.at[xx, zz], R.at[0, 0], sc.at[xx, zz], rc.at[0, 0], along("a", ar)).wait_send()
            remote(scales.at[xx, zz], RS.at[0, 0], ss.at[xx, zz], rs.at[0, 0], along("a", ar)).wait_send()
    for o in range(4):
        side, n = o % 2, o // 2
        remote(relay.at[side, n], R.at[0, 0], sf.at[side, n], rc.at[0, 0], along("a", ar)).wait_send()
        remote(relay_s.at[side, n], RS.at[0, 0], sfs.at[side, n], rs.at[0, 0], along("a", ar)).wait_send()
    save.wait()


def communicate(cot, bt, lengths, mom, rft):
    tok, rows = cot.shape
    feats = bt.shape[0]
    rank, cols = rft.shape
    tiles = cols // 128 * (rank // 8)
    half = tiles // 2
    n1, n2 = half // 8, half // 32
    return pl.pallas_call(
        comm_kernel,
        out_shape=(
            jax.ShapeDtypeStruct((rows, cols), f32),
            jax.ShapeDtypeStruct((tiles, 8, 128), f32),
            jax.ShapeDtypeStruct((rank, rank), f32),
            jax.ShapeDtypeStruct((rank, rows), f32),
        ),
        in_specs=[anyspec(), anyspec(), sspec(), anyspec(), anyspec()],
        out_specs=(anyspec(), vspec(), vspec(), vspec()),
        scratch_shapes=[
            VMEM((4, tok, rows), bf16),
            VMEM((4, feats, tok), bf16),
            VMEM((4, 4, feats, rows), jnp.int16),
            VMEM((4, 4, 8, rows), f32),
            VMEM((4, 4, feats, rows), jnp.int16),
            VMEM((4, 4, 8, rows), f32),
            VMEM((2, 2, feats, rows), jnp.int16),
            VMEM((2, 2, 8, rows), f32),
            VMEM((feats, rows), f32),
            VMEM((16, tok), bf16),
            VMEM((2 * feats, rows), f32),
            VMEM((2 * rank, cols), bf16),
            VMEM((rows, cols), f32),
            VMEM((rank, cols), f32),
            VMEM((rank, rows), f32),
            VMEM((rank, rows), f32),
            VMEM((4, rank, rows), f32),
            VMEM((2 * rank, rows), bf16),
            VMEM((tiles, 8, 128), f32),
            VMEM((half, 8, 128), f32),
            VMEM((2, 4, n1, 8, 128), f32),
            VMEM((2, 4, n2, 8, 128), f32),
            VMEM((2, 4, n2, 8, 128), f32),
            VMEM((4, rank, rank), f32),
            VMEM((4, rank, rank), f32),
            VMEM((rank, 2 * rank), f32),
            DMA((5,)), DMA((6,)), DMA((6,)), DMA((6,)), DMA((6,)),
            DMA((4, 4)), DMA((4, 4)), DMA((4, 4)), DMA((4, 4)),
            DMA((2, 2)), DMA((2, 2)), DMA((2, 2)), DMA((2, 2)),
            DMA((16, 4)), DMA((16, 4)),
        ],
        compiler_params=pltpu.CompilerParams(collective_id=0, has_side_effects=True),
        name="communicate",
    )(cot, bt, lengths, mom, rft)


def finish_kernel(
    coef, total, linv, left_t, both, weight, new_weight, new_mom, new_right_t,
    bv, wv, RT, R3, O3, NR, isem, osem,
):
    rows, cols = both.shape
    rank = linv.shape[0]
    wide = cols // 8

    def fetch(i):
        r = cols_of(i * wide, wide)
        return (
            pltpu.make_async_copy(both.at[:, r], bv.at[:, r], isem.at[i, 0]),
            pltpu.make_async_copy(weight.at[:, r], wv.at[:, r], isem.at[i, 1]),
        )

    def store(i):
        r = cols_of(i * wide, wide)
        return (
            pltpu.make_async_copy(bv.at[:, r], new_mom.at[:, r], osem.at[i, 0]),
            pltpu.make_async_copy(wv.at[:, r], new_weight.at[:, r], osem.at[i, 1]),
        )

    for i in range(8):
        for copy in fetch(i):
            copy.start()
    l_high, l_low = split(linv[...] * (1.0 / 8.0))

    def col(j, sq):
        high, low = split(jnp.concatenate([total[2 * j], total[2 * j + 1]], axis=1))
        v = dot(l_high, high) + dot(l_low, high) + dot(l_high, low)
        r = cols_of(j * 256, 256)
        RT[:, r] = v
        v_high, v_low = split(v)
        R3[0:rank, r] = v_high
        R3[rank : 2 * rank, r] = v_low
        R3[2 * rank : 3 * rank, r] = v_high
        return sq + v * v

    sq = lax.fori_loop(0, cols // 256, col, jnp.zeros((rank, 256), f32))
    norm = lax.rsqrt(jnp.sum(sq, axis=1, keepdims=True) + EPS)
    NR[...] = RT[...] * norm
    tell = pltpu.make_async_copy(NR, new_right_t, osem.at[8, 0])
    tell.start()
    ortho_t = jnp.dot(linv[...], left_t[...], precision=HI, preferred_element_type=f32)
    both_t = jnp.concatenate([ortho_t * (1.0 - MU), ortho_t * (norm * coef)], axis=1)
    o_high, o_low = split(both_t)
    O3[...] = jnp.concatenate([o_high, o_high, o_low], axis=0).T

    def work(i, carry):
        for copy in fetch(i):
            copy.wait()
        r = cols_of(i * wide, wide)
        low = dot(O3[...], R3[:, r])
        bv[:, r] = bv[:, r] - low[0:rows]
        wv[:, r] = (wv[:, r].astype(f32) - low[rows:]).astype(bf16)
        for copy in store(i):
            copy.start()
        return carry

    lax.fori_loop(0, 8, work, 0)
    for i in range(8):
        for copy in store(i):
            copy.wait()
    tell.wait()


def finish(coef, total, linv, left_t, both, weight):
    rows, cols = both.shape
    rank = linv.shape[0]
    return pl.pallas_call(
        functools.partial(finish_kernel, coef),
        out_shape=(
            jax.ShapeDtypeStruct((rows, cols), bf16),
            jax.ShapeDtypeStruct((rows, cols), f32),
            jax.ShapeDtypeStruct((rank, cols), f32),
        ),
        in_specs=[vspec(), vspec(), vspec(), anyspec(), anyspec()],
        out_specs=(anyspec(), anyspec(), anyspec()),
        scratch_shapes=[
            VMEM((rows, cols), f32),
            VMEM((rows, cols), bf16),
            VMEM((rank, cols), f32),
            VMEM((3 * rank, cols), bf16),
            VMEM((2 * rows, 3 * rank), bf16),
            VMEM((rank, cols), f32),
            DMA((8, 2)),
            DMA((9, 2)),
        ],
        name="finish",
    )(total, linv, left_t, both, weight)


def per_device(inputs, cotangent, lengths, momentum, weight, right_factor):
    both, total, linv, left_t = communicate(cotangent, inputs.T, lengths, momentum[0], right_factor.T)
    rank = linv.shape[0]
    rows_all = both.shape[0] * lax.axis_size("tensor")
    coef = LR * math.sqrt(rows_all / both.shape[1])
    new_weight, new_mom, new_right_t = finish(
        coef, total.reshape(-1, rank, 128), linv, left_t, both, weight
    )
    return (new_weight, new_mom[None], new_right_t.T)


def solution(mesh):
    placed = (
        P("dp", "tensor"),
        P("dp", "tensor"),
        P("dp"),
        P("dp", "tensor", None),
        P("tensor", None),
        P(),
    )
    return jax.shard_map(
        per_device,
        mesh=mesh,
        in_specs=placed,
        out_specs=(P("tensor", None), P("dp", "tensor", None), P()),
        check_vma=False,
    )
```

```python
import functools
import math

import jax
import jax.numpy as jnp
from jax import lax
from jax.experimental import pallas as pl
from jax.experimental.pallas import tpu as pltpu
from jax.sharding import PartitionSpec as P

EPS = 1e-06
MU = 0.95
LR = 0.02

f32 = jnp.float32
bf16 = jnp.bfloat16
HI = lax.Precision.HIGHEST
VMEM = pltpu.VMEM
DMA = pltpu.SemaphoreType.DMA
CODES = 32767.0
COMM_BYTES = 38 * 2**20
FINISH_BYTES = 16 * 2**20
DEPTH = 768


def vspec():
    return pl.BlockSpec(memory_space=pltpu.VMEM)


def hspec():
    return pl.BlockSpec(memory_space=pltpu.HBM)


def sspec():
    return pl.BlockSpec(memory_space=pltpu.SMEM)


def around(i, by):
    return lax.rem(i + by, 4)


def cols_of(start, size):
    return pl.ds(pl.multiple_of(start, 128), size)


def split(v):
    high = v.astype(bf16)
    return high, (v - high.astype(f32)).astype(bf16)


def dot(a, b, contract=((1,), (0,))):
    return lax.dot_general(a, b, (contract, ((), ())), preferred_element_type=f32)


def remote(src, dst, send, recv, where):
    return pltpu.make_async_remote_copy(
        src_ref=src,
        dst_ref=dst,
        send_sem=send,
        recv_sem=recv,
        device_id=where,
        device_id_type=pl.DeviceIdType.MESH,
    )


def greet(peers):
    barrier = pltpu.get_barrier_semaphore()
    for peer in peers:
        pl.semaphore_signal(barrier, inc=1, device_id=peer, device_id_type=pl.DeviceIdType.MESH)
    pl.semaphore_wait(barrier, len(peers))


def parts_of(tiles):
    most = tiles // 16 - 2 * (tiles // 48)
    return (most * 16, tiles // 48 * 16, tiles // 48 * 16)


def tile_column(tiles, j):
    return tiles[pl.ds(j * 8, 8)].reshape(64, 128)


def comm_kernel(
    cot, bt, lengths, mom, rft, both, RT, norm_out, ortho_out,
    A, B, codes, scales, R, RS, relay, relay_s, acc, keep, S, R2, rfv,
    LT, L0, L1, LL, LV, T, D, out, P1, P2, P3, G1, G2, M,
    sl, sa, ra, sb, rb, sc, ss, rc, rs, sf, sfs, rf, rfs, send, recv,
):
    t = lax.axis_index("tensor")
    d = lax.axis_index("dp")
    x, z = lax.div(t, 4), lax.rem(t, 4)
    y, c = lax.div(d, 2), lax.rem(d, 2)
    place = {"x": x, "y": y, "z": z}

    def along(axis, k):
        if axis == "core":
            return {"dp": y * 2 + k}
        if axis == "y":
            return {"dp": k * 2 + c}
        if axis == "x":
            return {"tensor": k * 4 + z}
        if axis == "z":
            return {"tensor": x * 4 + k}
        if axis == "a":
            return {"tensor": (1 - c) * (x * 4 + k) + c * (k * 4 + z)}
        return {"tensor": (1 - c) * (k * 4 + z) + c * (x * 4 + k)}

    pa = (1 - c) * z + c * x
    pb = (1 - c) * x + c * z
    al, ar, ao = around(pa, 3), around(pa, 1), around(pa, 2)
    bl, br, bo = around(pb, 3), around(pb, 1), around(pb, 2)
    tok, rows = cot.shape
    feats = bt.shape[0]
    ha, hb = tok // 2, feats // 2
    mate = along("core", 1 - c)

    locals_ = [
        pltpu.make_async_copy(cot, A.at[pa], sl.at[0]),
        pltpu.make_async_copy(bt, B.at[pb], sl.at[1]),
        pltpu.make_async_copy(mom, both, sl.at[2]),
        pltpu.make_async_copy(rft, rfv, sl.at[3]),
    ]
    greet([mate] + [along(a, around(place[a], q)) for a in "xyz" for q in (1, 2, 3)])

    def part_a(h):
        return pl.ds(h * ha, ha)

    def part_b(h):
        return pl.ds(h * hb, hb)

    sent = []
    for half, right in ((0, True), (1, False), (1, True), (0, False)):
        k = half + (0 if right else 2)
        ca = remote(cot.at[part_a(half)], A.at[pa, part_a(half)], sa.at[k], ra.at[k], along("a", ar if right else al))
        ca.start()
        cb = remote(bt.at[part_b(half)], B.at[pb, part_b(half)], sb.at[k], rb.at[k], along("b", br if right else bl))
        cb.start()
        sent += [ca, cb]
    for copy in locals_:
        copy.start()

    def got_a(k):
        remote(A.at[pa, part_a(0)], A.at[pa, part_a(0)], sa.at[0], ra.at[k], along("a", ar)).wait_recv()

    def got_b(k):
        remote(B.at[pb, part_b(0)], B.at[pb, part_b(0)], sb.at[0], rb.at[k], along("b", br)).wait_recv()

    def pass_a(k, half, origin, to):
        copy = remote(A.at[origin, part_a(half)], A.at[origin, part_a(half)], sa.at[k], ra.at[k], along("a", to))
        copy.start()
        sent.append(copy)

    def pass_b(k, half, origin, to):
        copy = remote(B.at[origin, part_b(half)], B.at[origin, part_b(half)], sb.at[k], rb.at[k], along("b", to))
        copy.start()
        sent.append(copy)

    block_len = tok // lengths.shape[0]
    count = lengths[0]
    for b in range(lengths.shape[0]):
        keep[:, b * block_len : (b + 1) * block_len] = (
            lax.broadcasted_iota(jnp.int32, (16, block_len), 1) < lengths[b]
        ).astype(f32).astype(bf16)
        if b:
            count = count + lengths[b]
    share = 1.0 / jnp.full((1, rows), count, jnp.int32).astype(f32)

    def unit(xx, zz, code_ref, scale_ref):
        acc[...] = jnp.zeros_like(acc)

        def step(k, carry):
            r = cols_of(k * DEPTH, DEPTH)
            acc[...] += dot(B[xx, :, r] * keep[0:1, r], A[zz, r, :])
            return carry

        lax.fori_loop(0, tok // DEPTH, step, 0)
        v = acc[...] * share
        top = jnp.max(jnp.abs(v), axis=0, keepdims=True)
        live = top > 1e-30
        code = jnp.round(v * jnp.where(live, CODES / jnp.where(live, top, 1.0), 0.0))
        code_ref[...] = code.astype(jnp.int32).astype(jnp.int16)
        scale_ref[...] = jnp.broadcast_to(jnp.where(live, top, 0.0) * (1.0 / CODES), (8, rows))

    def made(xx, zz):
        unit(xx, zz, codes.at[xx, zz], scales.at[xx, zz])

    def home(xx, zz):
        remote(codes.at[xx, zz], R.at[xx, pa], sc.at[xx, zz], rc.at[xx, pa], along("a", zz)).start()
        remote(scales.at[xx, zz], RS.at[xx, pa], ss.at[xx, zz], rs.at[xx, pa], along("a", zz)).start()

    def half_way(xx, side, n):
        to = along("a", around(pa, jnp.where(side == 0, 1, 3)))
        remote(codes.at[xx, ao], relay.at[side, n], sc.at[xx, ao], rf.at[side, n], to).start()
        remote(scales.at[xx, ao], relay_s.at[side, n], ss.at[xx, ao], rfs.at[side, n], to).start()

    def hand_on(o, wait_only=False):
        side, n = o % 2, o // 2
        xx = (pb, bl, br, bo)[o]
        origin, to = (al, ar) if side == 0 else (ar, al)
        one = remote(relay.at[side, n], R.at[xx, origin], sf.at[side, n], rf.at[side, n], along("a", to))
        one.wait_recv()
        two = remote(relay_s.at[side, n], RS.at[xx, origin], sfs.at[side, n], rfs.at[side, n], along("a", to))
        two.wait_recv()
        remote(relay.at[side, n], R.at[xx, origin], sf.at[side, n], rc.at[xx, origin], along("a", to)).start()
        remote(relay_s.at[side, n], RS.at[xx, origin], sfs.at[side, n], rs.at[xx, origin], along("a", to)).start()

    locals_[0].wait()
    locals_[1].wait()
    unit(pb, pa, R.at[pb, pa], RS.at[pb, pa])
    locals_[2].wait()
    locals_[3].wait()
    rank = rft.shape[0]
    r_high, r_low = split(rfv[...])
    R2[0:rank] = r_high
    R2[rank : 2 * rank] = r_low
    LT[...] = jnp.zeros_like(LT)

    def mom_left(g, carry):
        r = cols_of(g * 256, 256)
        high, low = split(both[:, r])
        v = dot(R2[:, r], high, ((1,), (1,)))
        LT[...] += v[0:rank] + v[rank:] + dot(R2[0:rank, r], low, ((1,), (1,)))
        return carry

    lax.fori_loop(0, both.shape[1] // 256, mom_left, 0)

    got_a(0)
    pass_a(4, 0, al, ar)
    got_a(3)
    pass_a(5, 1, ar, al)
    got_b(0)
    pass_b(4, 0, bl, br)
    got_b(3)
    pass_b(5, 1, br, bl)
    got_a(1)
    got_a(2)

    def own_cols(i, carry):
        zz = around(pa, 3 - 2 * i)
        made(pb, zz)
        home(pb, zz)
        return carry

    lax.fori_loop(0, 2, own_cols, 0)
    got_b(1)
    got_b(2)

    def next_cols(i, carry):
        xx = around(pb, 3 - 2 * lax.div(i, 3))
        m = lax.rem(i, 3)

        @pl.when(m == 2)
        def _():
            unit(xx, pa, R.at[xx, pa], RS.at[xx, pa])

        @pl.when(m != 2)
        def _():
            made(xx, around(pa, 3 - 2 * m))

        return carry

    lax.fori_loop(0, 6, next_cols, 0)
    got_a(4)
    got_a(5)

    def far_rows(i, carry):
        xx = around(pb, jnp.where(i == 0, 0, 5 - 2 * i))
        made(xx, ao)
        half_way(xx, lax.rem(i, 2), lax.div(i, 2))
        return carry

    lax.fori_loop(0, 3, far_rows, 0)
    for xx in (bl, br):
        home(xx, al)
        home(xx, ar)
    for o in range(3):
        hand_on(o)
    got_b(4)
    got_b(5)

    def far_cols(i, carry):
        @pl.when(i == 0)
        def _():
            made(bo, ao)
            half_way(bo, 1, 1)

        @pl.when(jnp.logical_and(i != 0, i != 3))
        def _():
            zz = around(pa, 5 - 2 * i)
            made(bo, zz)
            home(bo, zz)

        @pl.when(i == 3)
        def _():
            unit(bo, pa, R.at[bo, pa], RS.at[bo, pa])

        return carry

    lax.fori_loop(0, 4, far_cols, 0)
    hand_on(3)

    late = lax.div(bo, 2)

    def gather_home(n, carry):
        o, h = lax.div(n, 2), lax.rem(n, 2)
        xx = around(pb, jnp.where(o == 0, 0, jnp.where(o == 3, 2, 5 - 2 * o)))
        group = jnp.where(n < 4, 1 - late, late)
        base = jnp.where(c == 0, xx * 2 + h, lax.rem(n, 4) * 2 + group) * (2 * feats)
        for i in range(2):
            xi = jnp.where(c == 0, xx, 2 * group + i)
            zi = jnp.where(c == 0, 2 * h + i, lax.rem(n, 4))

            @pl.when(zi != pa)
            def _():
                remote(codes.at[0, 0], R.at[xi, zi], sc.at[0, 0], rc.at[xi, zi], along("a", ar)).wait_recv()
                remote(scales.at[0, 0], RS.at[xi, zi], ss.at[0, 0], rs.at[xi, zi], along("a", ar)).wait_recv()

            S[i * feats : (i + 1) * feats] = R[xi, zi].astype(jnp.int32).astype(f32) * RS[xi, zi, 0:1]
        high, low = split(S[...])
        r = cols_of(base, 2 * feats)
        v = dot(R2[:, r], high)
        LT[...] += v[0:rank] + v[rank:] + dot(R2[0:rank, r], low)
        for i in range(2 * feats // 128):
            both[:, cols_of(base + 128 * i, 128)] += S[128 * i : 128 * (i + 1)].T
        return carry

    lax.fori_loop(0, 8, gather_home, 0)

    pending = []

    def swap(stage, src, dst):
        copy = remote(src, dst, send.at[stage, 0], recv.at[stage, 0], mate)
        copy.start()
        pending.append(copy)
        return copy

    def spread(stage, axis, src, dst):
        me = place[axis]
        waits = []
        for q in (2, 1, 3):
            k = around(me, q)
            copy = remote(src(k), dst(me), send.at[stage, q], recv.at[stage, q], along(axis, k))
            copy.start()
            pending.append(copy)
            waits.append(remote(src(k), dst(around(me, 4 - q)), send.at[stage, q], recv.at[stage, q], along(axis, k)))

        def wait():
            for w in waits:
                w.wait_recv()

        return wait

    swap(0, LT, L0).wait_recv()
    L1[y] = LT[...] + L0[...]
    spread(1, "y", lambda k: L1.at[y], lambda k: L1.at[k])()
    left = (L1[0] + L1[1] + L1[2] + L1[3]) * (1.0 / 8.0)
    left_high, left_low = split(left)
    LL[0:rank] = left_high
    LL[rank : 2 * rank] = left_low
    v = dot(LL[...], left_high, ((1,), (1,)))
    G1[z] = v[0:rank] + v[rank:] + dot(left_high, left_low, ((1,), (1,)))
    gram_wait = spread(2, "z", lambda k: G1.at[z], lambda k: G1.at[k])

    tiles = both.shape[1] // 128 * (rank // 8)
    half = tiles // 2
    blocks = both.shape[1] // 512

    def block(g, carry):
        high, low = split(both[:, cols_of(g * 256, 256)])
        v = dot(LL[...], high)
        v = v[0:rank] + v[rank:] + dot(LL[0:rank], low)
        for i in range(2):
            T[pl.ds(g * 16 + i * 8, 8)] = v[:, 128 * i : 128 * (i + 1)].reshape(8, 8, 128)
        return carry

    lax.fori_loop(blocks * (1 - c), blocks * (2 - c), block, 0)
    mine, theirs = c * half, (1 - c) * half
    core_wait = swap(3, T.at[pl.ds(theirs, half)], D)
    lax.fori_loop(blocks * c, blocks * (1 + c), block, 0)
    core_wait.wait_recv()

    def add_core(g, carry):
        r = pl.ds(mine + g * 20, 20)
        T[r] = T[r] + D[pl.ds(g * 20, 20)]
        return carry

    lax.fori_loop(0, half // 20, add_core, 0)

    orders = (("y", "x", "z"), ("x", "z", "y"), ("z", "y", "x"))
    sizes = parts_of(half)
    base = [mine, mine + sizes[0], mine + sizes[0] + sizes[1]]
    n1 = [size // 4 for size in sizes]
    n2 = [size // 16 for size in sizes]
    zeroth, first, second, third, fourth = [], [], [], [], []
    for k, (a1, a2, a3) in enumerate(orders):
        zeroth.append(
            spread(
                4 + k, a1,
                lambda q, k=k: T.at[pl.ds(base[k] + q * n1[k], n1[k])],
                lambda q, k=k: P1.at[k, q, 0 : n1[k]],
            )
        )
    gram_wait()
    G2[x] = G1[0] + G1[1] + G1[2] + G1[3]
    gram_wait = spread(19, "x", lambda k: G2.at[x], lambda k: G2.at[k])
    for k, (a1, a2, a3) in enumerate(orders):
        me = place[a1]
        P1[k, me, 0 : n1[k]] = T[pl.ds(base[k] + me * n1[k], n1[k])]
        zeroth[k]()
        low = slice(0, n1[k])
        P1[k, 0, low] = P1[k, 0, low] + P1[k, 1, low] + P1[k, 2, low] + P1[k, 3, low]
        first.append(
            spread(
                7 + k, a2,
                lambda q, k=k: P1.at[k, 0, pl.ds(q * n2[k], n2[k])],
                lambda q, k=k: P2.at[k, q, 0 : n2[k]],
            )
        )
    row_id = lax.broadcasted_iota(jnp.int32, (rank, 2 * rank), 0)
    lane_id = lax.broadcasted_iota(jnp.int32, (rank, 2 * rank), 1)
    gram_wait()
    M[...] = jnp.where(lane_id == row_id + rank, 1.0, 0.0)
    M[:, 0:rank] = G2[0] + G2[1] + G2[2] + G2[3]

    def pivot(k, carry):
        m = M[...]
        row = M[pl.ds(k, 1), :]
        top = jnp.sum(jnp.where(lane_id[0:1] == k, row, 0.0), axis=1, keepdims=True)
        factor = jnp.sum(jnp.where(lane_id == k, m, 0.0), axis=1, keepdims=True)
        factor = jnp.where(row_id[:, 0:1] > k, factor / top, 0.0)
        M[...] = m - factor * row
        return carry

    cuts = (0, 16, 32, 48, rank)
    lax.fori_loop(cuts[0], cuts[1], pivot, 0)
    for k, (a1, a2, a3) in enumerate(orders):
        me = place[a2]
        low = slice(0, n2[k])
        P2[k, me, low] = P1[k, 0, pl.ds(me * n2[k], n2[k])]
        first[k]()
        m3 = place[a3]
        P3[k, m3, low] = P2[k, 0, low] + P2[k, 1, low] + P2[k, 2, low] + P2[k, 3, low]
        second.append(
            spread(
                10 + k, a3,
                lambda q, k=k, m3=m3: P3.at[k, m3, 0 : n2[k]],
                lambda q, k=k: P3.at[k, q, 0 : n2[k]],
            )
        )
    lax.fori_loop(cuts[1], cuts[2], pivot, 0)
    for k, (a1, a2, a3) in enumerate(orders):
        second[k]()
        row = base[k] + place[a1] * n1[k]
        spot = row + place[a2] * n2[k]
        low = slice(0, n2[k])
        out[pl.ds(spot, n2[k])] = P3[k, 0, low] + P3[k, 1, low] + P3[k, 2, low] + P3[k, 3, low]
        third.append(
            spread(
                13 + k, a2,
                lambda q, spot=spot, k=k: out.at[pl.ds(spot, n2[k])],
                lambda q, row=row, k=k: out.at[pl.ds(row + q * n2[k], n2[k])],
            )
        )
    lax.fori_loop(cuts[2], cuts[3], pivot, 0)
    for k, (a1, a2, a3) in enumerate(orders):
        third[k]()
        row = base[k] + place[a1] * n1[k]
        fourth.append(
            spread(
                16 + k, a1,
                lambda q, row=row, k=k: out.at[pl.ds(row, n1[k])],
                lambda q, k=k: out.at[pl.ds(base[k] + q * n1[k], n1[k])],
            )
        )
    lax.fori_loop(cuts[3], cuts[4], pivot, 0)
    m = M[...]
    diag = jnp.sum(jnp.where(lane_id == row_id, m, 0.0), axis=1, keepdims=True)
    linv = pltpu.roll(m / jnp.sqrt(diag), rank, 1)[:, 0:rank]
    ortho_out[...] = jnp.dot(linv, (L1[0] + L1[1] + L1[2] + L1[3]) * (1.0 / 8.0), precision=HI, preferred_element_type=f32)
    v_high, v_low = split(linv * (1.0 / 8.0))
    LV[0] = v_high
    LV[1] = v_low
    for k in range(3):
        fourth[k]()
    swap(20, out.at[pl.ds(mine, half)], out.at[pl.ds(mine, half)])

    def right(j, sq):
        high, low = split(jnp.concatenate([tile_column(out, 2 * j), tile_column(out, 2 * j + 1)], axis=1))
        v = dot(LV[0], high) + dot(LV[1], high) + dot(LV[0], low)
        RT[:, cols_of(j * 256, 256)] = v
        return sq + v * v

    sq = lax.fori_loop(blocks * c, blocks * (1 + c), right, jnp.zeros((rank, 256), f32))
    remote(out.at[pl.ds(theirs, half)], out.at[pl.ds(theirs, half)], send.at[20, 0], recv.at[20, 0], mate).wait_recv()
    sq_other = lax.fori_loop(blocks * (1 - c), blocks * (2 - c), right, jnp.zeros((rank, 256), f32))
    total = jnp.where(c == 0, sq, sq_other) + jnp.where(c == 0, sq_other, sq)
    norm = lax.rsqrt(jnp.sum(total, axis=1, keepdims=True) + EPS)
    norm_out[...] = jnp.broadcast_to(norm, norm_out.shape)

    for copy in pending + sent:
        copy.wait_send()
    for by in (1, 2, 3):
        for xx in range(4):
            zz = around(pa, by)
            remote(codes.at[xx, zz], R.at[0, 0], sc.at[xx, zz], rc.at[0, 0], along("a", ar)).wait_send()
            remote(scales.at[xx, zz], RS.at[0, 0], ss.at[xx, zz], rs.at[0, 0], along("a", ar)).wait_send()
    for o in range(4):
        side, n = o % 2, o // 2
        remote(relay.at[side, n], R.at[0, 0], sf.at[side, n], rc.at[0, 0], along("a", ar)).wait_send()
        remote(relay_s.at[side, n], RS.at[0, 0], sfs.at[side, n], rs.at[0, 0], along("a", ar)).wait_send()


def communicate(cot, bt, lengths, mom, rft):
    tok, rows = cot.shape
    feats = bt.shape[0]
    rank, cols = rft.shape
    tiles = cols // 128 * (rank // 8)
    half = tiles // 2
    most = max(parts_of(half))
    n1, n2 = most // 4, most // 16
    return pl.pallas_call(
        comm_kernel,
        out_shape=(
            jax.ShapeDtypeStruct((rows, cols), f32),
            jax.ShapeDtypeStruct((rank, cols), f32),
            jax.ShapeDtypeStruct((rank, 128), f32),
            jax.ShapeDtypeStruct((rank, rows), f32),
        ),
        in_specs=[hspec(), hspec(), sspec(), hspec(), hspec()],
        out_specs=(vspec(), vspec(), vspec(), vspec()),
        scratch_shapes=[
            VMEM((4, tok, rows), bf16),
            VMEM((4, feats, tok), bf16),
            VMEM((4, 4, feats, rows), jnp.int16),
            VMEM((4, 4, 8, rows), f32),
            VMEM((4, 4, feats, rows), jnp.int16),
            VMEM((4, 4, 8, rows), f32),
            VMEM((2, 2, feats, rows), jnp.int16),
            VMEM((2, 2, 8, rows), f32),
            VMEM((feats, rows), f32),
            VMEM((16, tok), bf16),
            VMEM((2 * feats, rows), f32),
            VMEM((2 * rank, cols), bf16),
            VMEM((rank, cols), f32),
            VMEM((rank, rows), f32),
            VMEM((rank, rows), f32),
            VMEM((4, rank, rows), f32),
            VMEM((2 * rank, rows), bf16),
            VMEM((2, rank, rank), bf16),
            VMEM((tiles, 8, 128), f32),
            VMEM((half, 8, 128), f32),
            VMEM((tiles, 8, 128), f32),
            VMEM((3, 4, n1, 8, 128), f32),
            VMEM((3, 4, n2, 8, 128), f32),
            VMEM((3, 4, n2, 8, 128), f32),
            VMEM((4, rank, rank), f32),
            VMEM((4, rank, rank), f32),
            VMEM((rank, 2 * rank), f32),
            DMA((5,)), DMA((6,)), DMA((6,)), DMA((6,)), DMA((6,)),
            DMA((4, 4)), DMA((4, 4)), DMA((4, 4)), DMA((4, 4)),
            DMA((2, 2)), DMA((2, 2)), DMA((2, 2)), DMA((2, 2)),
            DMA((21, 4)), DMA((21, 4)),
        ],
        compiler_params=pltpu.CompilerParams(
            collective_id=0, has_side_effects=True, vmem_limit_bytes=COMM_BYTES
        ),
        name="communicate",
    )(cot, bt, lengths, mom, rft)


def finish_kernel(
    coef, right_t, norm, ortho_t, both, weight, new_weight, new_mom, new_right_t,
    bv, wv, NR, O3, osem,
):
    rows, cols = both.shape
    wide = cols // 8

    def store(i):
        r = cols_of(i * wide, wide)
        return (
            pltpu.make_async_copy(bv.at[:, r], new_mom.at[:, r], osem.at[i, 0]),
            pltpu.make_async_copy(wv.at[:, r], new_weight.at[:, r], osem.at[i, 1]),
            pltpu.make_async_copy(NR.at[:, r], new_right_t.at[:, r], osem.at[i, 2]),
        )

    both_t = jnp.concatenate([ortho_t[...] * (1.0 - MU), ortho_t[...] * (norm[:, 0:1] * coef)], axis=1)
    o_high, o_low = split(both_t)
    O3[...] = jnp.concatenate([o_high, o_high, o_low], axis=0).T

    def work(i, carry):
        r = cols_of(i * wide, wide)
        v = right_t[:, r]
        high, low = split(v)
        change = dot(O3[...], jnp.concatenate([high, low, high], axis=0))
        bv[:, r] = both[:, r] - change[0:rows]
        wv[:, r] = (weight[:, r].astype(f32) - change[rows:]).astype(bf16)
        NR[:, r] = v * norm[:, 0:1]
        for copy in store(i):
            copy.start()
        return carry

    lax.fori_loop(0, 8, work, 0)
    for i in range(8):
        for copy in store(i):
            copy.wait()


def finish(coef, right_t, norm, ortho_t, both, weight):
    rows, cols = both.shape
    rank = right_t.shape[0]
    return pl.pallas_call(
        functools.partial(finish_kernel, coef),
        out_shape=(
            jax.ShapeDtypeStruct((rows, cols), bf16),
            jax.ShapeDtypeStruct((rows, cols), f32),
            jax.ShapeDtypeStruct((rank, cols), f32),
        ),
        in_specs=[vspec()] * 5,
        out_specs=(hspec(), hspec(), hspec()),
        scratch_shapes=[
            VMEM((rows, cols), f32),
            VMEM((rows, cols), bf16),
            VMEM((rank, cols), f32),
            VMEM((2 * rows, 3 * rank), bf16),
            DMA((8, 3)),
        ],
        compiler_params=pltpu.CompilerParams(vmem_limit_bytes=FINISH_BYTES),
        name="finish",
    )(right_t, norm, ortho_t, both, weight)


def per_device(inputs, cotangent, lengths, momentum, weight, right_factor):
    stay = lambda v: pltpu.with_memory_space_constraint(v, pltpu.HBM)
    both, right_t, norm, ortho_t = communicate(
        stay(cotangent), stay(inputs.T), stay(lengths), stay(momentum[0]), stay(right_factor.T)
    )
    rows_all = both.shape[0] * lax.axis_size("tensor")
    coef = LR * math.sqrt(rows_all / both.shape[1])
    new_weight, new_mom, new_right_t = finish(coef, right_t, norm, ortho_t, both, weight)
    return (new_weight, new_mom[None], new_right_t.T)


def solution(mesh):
    placed = (
        P("dp", "tensor"),
        P("dp", "tensor"),
        P("dp"),
        P("dp", "tensor", None),
        P("tensor", None),
        P(),
    )
    return jax.shard_map(
        per_device,
        mesh=mesh,
        in_specs=placed,
        out_specs=(P("tensor", None), P("dp", "tensor", None), P()),
        check_vma=False,
    )
```

```python
import functools
import math

import jax
import jax.numpy as jnp
from jax import lax
from jax.experimental import pallas as pl
from jax.experimental.pallas import tpu as pltpu
from jax.sharding import PartitionSpec as P

EPS = 1e-06
MU = 0.95
LR = 0.02

f32 = jnp.float32
bf16 = jnp.bfloat16
HI = lax.Precision.HIGHEST
VMEM = pltpu.VMEM
DMA = pltpu.SemaphoreType.DMA
CODES = 32767.0
COMM_BYTES = 38 * 2**20
FINISH_BYTES = 16 * 2**20
DEPTH = 768


def vspec():
    return pl.BlockSpec(memory_space=pltpu.VMEM)


def hspec():
    return pl.BlockSpec(memory_space=pltpu.HBM)


def sspec():
    return pl.BlockSpec(memory_space=pltpu.SMEM)


def around(i, by):
    return lax.rem(i + by, 4)


def cols_of(start, size):
    return pl.ds(pl.multiple_of(start, 128), size)


def split(v):
    high = v.astype(bf16)
    return high, (v - high.astype(f32)).astype(bf16)


def dot(a, b, contract=((1,), (0,))):
    return lax.dot_general(a, b, (contract, ((), ())), preferred_element_type=f32)


def remote(src, dst, send, recv, where):
    return pltpu.make_async_remote_copy(
        src_ref=src,
        dst_ref=dst,
        send_sem=send,
        recv_sem=recv,
        device_id=where,
        device_id_type=pl.DeviceIdType.MESH,
    )


def greet(peers):
    barrier = pltpu.get_barrier_semaphore()
    for peer in peers:
        pl.semaphore_signal(barrier, inc=1, device_id=peer, device_id_type=pl.DeviceIdType.MESH)
    pl.semaphore_wait(barrier, len(peers))


def parts_of(tiles):
    most = tiles // 16 - 2 * (tiles // 48)
    return (most * 16, tiles // 48 * 16, tiles // 48 * 16)


def tile_column(tiles, j):
    return tiles[pl.ds(j * 8, 8)].reshape(64, 128)


def comm_kernel(
    cot, bt, lengths, mom, rft, both, RT, norm_out, ortho_out,
    A, B, codes, scales, R, RS, relay, relay_s, acc, keep, S, R2, rfv,
    LT, L0, L1, LL, LV, T, D, out, P1, P2, P3, G1, G2, M,
    sl, sa, ra, sb, rb, sc, ss, rc, rs, sf, sfs, rf, rfs, send, recv,
):
    t = lax.axis_index("tensor")
    d = lax.axis_index("dp")
    x, z = lax.div(t, 4), lax.rem(t, 4)
    y, c = lax.div(d, 2), lax.rem(d, 2)
    place = {"x": x, "y": y, "z": z}

    def along(axis, k):
        if axis == "core":
            return {"dp": y * 2 + k}
        if axis == "y":
            return {"dp": k * 2 + c}
        if axis == "x":
            return {"tensor": k * 4 + z}
        if axis == "z":
            return {"tensor": x * 4 + k}
        if axis == "a":
            return {"tensor": (1 - c) * (x * 4 + k) + c * (k * 4 + z)}
        return {"tensor": (1 - c) * (k * 4 + z) + c * (x * 4 + k)}

    pa = (1 - c) * z + c * x
    pb = (1 - c) * x + c * z
    al, ar, ao = around(pa, 3), around(pa, 1), around(pa, 2)
    bl, br, bo = around(pb, 3), around(pb, 1), around(pb, 2)
    tok, rows = cot.shape
    feats = bt.shape[0]
    ha, hb = tok // 2, feats // 2
    mate = along("core", 1 - c)

    locals_ = [
        pltpu.make_async_copy(cot, A.at[pa], sl.at[0]),
        pltpu.make_async_copy(bt, B.at[pb], sl.at[1]),
        pltpu.make_async_copy(mom, both, sl.at[2]),
        pltpu.make_async_copy(rft, rfv, sl.at[3]),
    ]
    greet([mate] + [along(a, around(place[a], q)) for a in "xyz" for q in (1, 2, 3)])

    def part_a(h):
        return pl.ds(h * ha, ha)

    def part_b(h):
        return pl.ds(h * hb, hb)

    sent = []
    for half, right in ((0, True), (1, False), (1, True), (0, False)):
        k = half + (0 if right else 2)
        ca = remote(cot.at[part_a(half)], A.at[pa, part_a(half)], sa.at[k], ra.at[k], along("a", ar if right else al))
        ca.start()
        cb = remote(bt.at[part_b(half)], B.at[pb, part_b(half)], sb.at[k], rb.at[k], along("b", br if right else bl))
        cb.start()
        sent += [ca, cb]
    for copy in locals_:
        copy.start()

    def got_a(k):
        remote(A.at[pa, part_a(0)], A.at[pa, part_a(0)], sa.at[0], ra.at[k], along("a", ar)).wait_recv()

    def got_b(k):
        remote(B.at[pb, part_b(0)], B.at[pb, part_b(0)], sb.at[0], rb.at[k], along("b", br)).wait_recv()

    def pass_a(k, half, origin, to):
        copy = remote(A.at[origin, part_a(half)], A.at[origin, part_a(half)], sa.at[k], ra.at[k], along("a", to))
        copy.start()
        sent.append(copy)

    def pass_b(k, half, origin, to):
        copy = remote(B.at[origin, part_b(half)], B.at[origin, part_b(half)], sb.at[k], rb.at[k], along("b", to))
        copy.start()
        sent.append(copy)

    block_len = tok // lengths.shape[0]
    count = lengths[0]
    for b in range(lengths.shape[0]):
        keep[:, b * block_len : (b + 1) * block_len] = (
            lax.broadcasted_iota(jnp.int32, (16, block_len), 1) < lengths[b]
        ).astype(f32).astype(bf16)
        if b:
            count = count + lengths[b]
    share = 1.0 / jnp.full((1, rows), count, jnp.int32).astype(f32)

    def unit(xx, zz, code_ref, scale_ref):
        acc[...] = jnp.zeros_like(acc)

        def step(k, carry):
            r = cols_of(k * DEPTH, DEPTH)
            acc[...] += dot(B[xx, :, r] * keep[0:1, r], A[zz, r, :])
            return carry

        lax.fori_loop(0, tok // DEPTH, step, 0)
        v = acc[...] * share
        top = jnp.max(jnp.abs(v), axis=0, keepdims=True)
        live = top > 1e-30
        code = jnp.round(v * jnp.where(live, CODES / jnp.where(live, top, 1.0), 0.0))
        code_ref[...] = code.astype(jnp.int32).astype(jnp.int16)
        scale_ref[...] = jnp.broadcast_to(jnp.where(live, top, 0.0) * (1.0 / CODES), (8, rows))

    def made(xx, zz):
        unit(xx, zz, codes.at[xx, zz], scales.at[xx, zz])

    def home(xx, zz):
        remote(codes.at[xx, zz], R.at[xx, pa], sc.at[xx, zz], rc.at[xx, pa], along("a", zz)).start()
        remote(scales.at[xx, zz], RS.at[xx, pa], ss.at[xx, zz], rs.at[xx, pa], along("a", zz)).start()

    def half_way(xx, side, n):
        to = along("a", around(pa, jnp.where(side == 0, 1, 3)))
        remote(codes.at[xx, ao], relay.at[side, n], sc.at[xx, ao], rf.at[side, n], to).start()
        remote(scales.at[xx, ao], relay_s.at[side, n], ss.at[xx, ao], rfs.at[side, n], to).start()

    def hand_on(o, wait_only=False):
        side, n = o % 2, o // 2
        xx = (pb, bl, br, bo)[o]
        origin, to = (al, ar) if side == 0 else (ar, al)
        one = remote(relay.at[side, n], R.at[xx, origin], sf.at[side, n], rf.at[side, n], along("a", to))
        one.wait_recv()
        two = remote(relay_s.at[side, n], RS.at[xx, origin], sfs.at[side, n], rfs.at[side, n], along("a", to))
        two.wait_recv()
        remote(relay.at[side, n], R.at[xx, origin], sf.at[side, n], rc.at[xx, origin], along("a", to)).start()
        remote(relay_s.at[side, n], RS.at[xx, origin], sfs.at[side, n], rs.at[xx, origin], along("a", to)).start()

    locals_[0].wait()
    locals_[1].wait()
    unit(pb, pa, R.at[pb, pa], RS.at[pb, pa])
    locals_[2].wait()
    locals_[3].wait()
    rank = rft.shape[0]
    r_high, r_low = split(rfv[...])
    R2[0:rank] = r_high
    R2[rank : 2 * rank] = r_low
    LT[...] = jnp.zeros_like(LT)

    def mom_left(g, carry):
        r = cols_of(g * 256, 256)
        high, low = split(both[:, r])
        v = dot(R2[:, r], high, ((1,), (1,)))
        LT[...] += v[0:rank] + v[rank:] + dot(R2[0:rank, r], low, ((1,), (1,)))
        return carry

    lax.fori_loop(0, both.shape[1] // 256, mom_left, 0)

    got_a(0)
    pass_a(4, 0, al, ar)
    got_a(3)
    pass_a(5, 1, ar, al)
    got_b(0)
    pass_b(4, 0, bl, br)
    got_b(3)
    pass_b(5, 1, br, bl)
    got_a(1)
    got_a(2)

    def own_cols(i, carry):
        zz = around(pa, 3 - 2 * i)
        made(pb, zz)
        home(pb, zz)
        return carry

    lax.fori_loop(0, 2, own_cols, 0)
    got_b(1)
    got_b(2)

    def next_cols(i, carry):
        xx = around(pb, 3 - 2 * lax.div(i, 3))
        m = lax.rem(i, 3)

        @pl.when(m == 2)
        def _():
            unit(xx, pa, R.at[xx, pa], RS.at[xx, pa])

        @pl.when(m != 2)
        def _():
            made(xx, around(pa, 3 - 2 * m))

        return carry

    lax.fori_loop(0, 6, next_cols, 0)
    got_a(4)
    got_a(5)

    def far_rows(i, carry):
        xx = around(pb, jnp.where(i == 0, 0, 5 - 2 * i))
        made(xx, ao)
        half_way(xx, lax.rem(i, 2), lax.div(i, 2))
        return carry

    lax.fori_loop(0, 3, far_rows, 0)
    for xx in (bl, br):
        home(xx, al)
        home(xx, ar)
    for o in range(3):
        hand_on(o)
    got_b(4)
    got_b(5)

    def far_cols(i, carry):
        @pl.when(i == 0)
        def _():
            made(bo, ao)
            half_way(bo, 1, 1)

        @pl.when(jnp.logical_and(i != 0, i != 3))
        def _():
            zz = around(pa, 5 - 2 * i)
            made(bo, zz)
            home(bo, zz)

        @pl.when(i == 3)
        def _():
            unit(bo, pa, R.at[bo, pa], RS.at[bo, pa])

        return carry

    lax.fori_loop(0, 4, far_cols, 0)
    late, far = lax.div(bo, 2), lax.div(ao, 2)

    def gather_home(n, carry):
        o = jnp.where(n < 6, lax.rem(n, 3), 3)
        h = jnp.where(jnp.logical_or(n < 3, n == 6), 1 - far, far)
        xx = around(pb, jnp.where(o == 0, 0, jnp.where(o == 3, 2, 5 - 2 * o)))
        group = jnp.where(n < 4, 1 - late, late)
        m = lax.rem(n, 4)
        zz = around(pa, jnp.where(m == 0, 0, jnp.where(m == 3, 2, 5 - 2 * m)))
        base = jnp.where(c == 0, xx * 2 + h, zz * 2 + group) * (2 * feats)
        for i in range(2):
            xi = jnp.where(c == 0, xx, 2 * group + i)
            zi = jnp.where(c == 0, 2 * h + i, zz)

            @pl.when(zi != pa)
            def _():
                remote(codes.at[0, 0], R.at[xi, zi], sc.at[0, 0], rc.at[xi, zi], along("a", ar)).wait_recv()
                remote(scales.at[0, 0], RS.at[xi, zi], ss.at[0, 0], rs.at[xi, zi], along("a", ar)).wait_recv()

            S[i * feats : (i + 1) * feats] = R[xi, zi].astype(jnp.int32).astype(f32) * RS[xi, zi, 0:1]
        high, low = split(S[...])
        r = cols_of(base, 2 * feats)
        v = dot(R2[:, r], high)
        LT[...] += v[0:rank] + v[rank:] + dot(R2[0:rank, r], low)
        for i in range(2 * feats // 128):
            both[:, cols_of(base + 128 * i, 128)] += S[128 * i : 128 * (i + 1)].T
        return carry

    lax.fori_loop(0, 3, gather_home, 0)
    hand_on(3)
    lax.fori_loop(3, 8, gather_home, 0)

    pending = []

    def swap(stage, src, dst, k=0):
        copy = remote(src, dst, send.at[stage, k], recv.at[stage, k], mate)
        copy.start()
        pending.append(copy)
        return copy

    def spread(stage, axis, src, dst):
        me = place[axis]
        waits = []
        for q in (2, 1, 3):
            k = around(me, q)
            copy = remote(src(k), dst(me), send.at[stage, q], recv.at[stage, q], along(axis, k))
            copy.start()
            pending.append(copy)
            waits.append(remote(src(k), dst(around(me, 4 - q)), send.at[stage, q], recv.at[stage, q], along(axis, k)))

        def wait():
            for w in waits:
                w.wait_recv()

        return wait

    swap(0, LT, L0).wait_recv()
    L1[y] = LT[...] + L0[...]
    spread(1, "y", lambda k: L1.at[y], lambda k: L1.at[k])()
    left = (L1[0] + L1[1] + L1[2] + L1[3]) * (1.0 / 8.0)
    left_high, left_low = split(left)
    LL[0:rank] = left_high
    LL[rank : 2 * rank] = left_low
    v = dot(LL[...], left_high, ((1,), (1,)))
    G1[z] = v[0:rank] + v[rank:] + dot(left_high, left_low, ((1,), (1,)))
    gram_wait = spread(2, "z", lambda k: G1.at[z], lambda k: G1.at[k])

    tiles = both.shape[1] // 128 * (rank // 8)
    half = tiles // 2
    blocks = both.shape[1] // 512

    def block(g, carry):
        high, low = split(both[:, cols_of(g * 256, 256)])
        v = dot(LL[...], high)
        v = v[0:rank] + v[rank:] + dot(LL[0:rank], low)
        for i in range(2):
            T[pl.ds(g * 16 + i * 8, 8)] = v[:, 128 * i : 128 * (i + 1)].reshape(8, 8, 128)
        return carry

    orders = (("y", "x", "z"), ("x", "z", "y"), ("z", "y", "x"))
    sizes = parts_of(half)
    begin = (0, sizes[0], sizes[0] + sizes[1])
    mine, theirs = c * half, (1 - c) * half
    base = [mine + start for start in begin]
    n1 = [size // 4 for size in sizes]
    n2 = [size // 16 for size in sizes]

    def part_blocks(side, k):
        start = blocks * side + begin[k] // 16
        return start, start + sizes[k] // 16

    core_waits = []
    for k in range(3):
        lax.fori_loop(*part_blocks(1 - c, k), block, 0)
        core_waits.append(
            swap(3, T.at[pl.ds(theirs + begin[k], sizes[k])], D.at[pl.ds(begin[k], sizes[k])], k)
        )

    def add_core(g, carry):
        r = pl.ds(mine + g * 16, 16)
        T[r] = T[r] + D[pl.ds(g * 16, 16)]
        return carry

    zeroth, first, second, third, fourth = [], [], [], [], []
    for k, (a1, a2, a3) in enumerate(orders):
        lax.fori_loop(*part_blocks(c, k), block, 0)
        core_waits[k].wait_recv()
        lax.fori_loop(begin[k] // 16, (begin[k] + sizes[k]) // 16, add_core, 0)
        zeroth.append(
            spread(
                4 + k, a1,
                lambda q, k=k: T.at[pl.ds(base[k] + q * n1[k], n1[k])],
                lambda q, k=k: P1.at[k, q, 0 : n1[k]],
            )
        )
    gram_wait()
    G2[x] = G1[0] + G1[1] + G1[2] + G1[3]
    gram_wait = spread(19, "x", lambda k: G2.at[x], lambda k: G2.at[k])
    for k, (a1, a2, a3) in enumerate(orders):
        me = place[a1]
        P1[k, me, 0 : n1[k]] = T[pl.ds(base[k] + me * n1[k], n1[k])]
        zeroth[k]()
        low = slice(0, n1[k])
        P1[k, 0, low] = P1[k, 0, low] + P1[k, 1, low] + P1[k, 2, low] + P1[k, 3, low]
        first.append(
            spread(
                7 + k, a2,
                lambda q, k=k: P1.at[k, 0, pl.ds(q * n2[k], n2[k])],
                lambda q, k=k: P2.at[k, q, 0 : n2[k]],
            )
        )
    row_id = lax.broadcasted_iota(jnp.int32, (rank, 2 * rank), 0)
    lane_id = lax.broadcasted_iota(jnp.int32, (rank, 2 * rank), 1)
    gram_wait()
    M[...] = jnp.where(lane_id == row_id + rank, 1.0, 0.0)
    M[:, 0:rank] = G2[0] + G2[1] + G2[2] + G2[3]

    def pivot(k, carry):
        m = M[...]
        row = M[pl.ds(k, 1), :]
        top = jnp.sum(jnp.where(lane_id[0:1] == k, row, 0.0), axis=1, keepdims=True)
        factor = jnp.sum(jnp.where(lane_id == k, m, 0.0), axis=1, keepdims=True)
        factor = jnp.where(row_id[:, 0:1] > k, factor / top, 0.0)
        M[...] = m - factor * row
        return carry

    cuts = (0, 16, 32, 48, rank)
    lax.fori_loop(cuts[0], cuts[1], pivot, 0)
    for k, (a1, a2, a3) in enumerate(orders):
        me = place[a2]
        low = slice(0, n2[k])
        P2[k, me, low] = P1[k, 0, pl.ds(me * n2[k], n2[k])]
        first[k]()
        m3 = place[a3]
        P3[k, m3, low] = P2[k, 0, low] + P2[k, 1, low] + P2[k, 2, low] + P2[k, 3, low]
        second.append(
            spread(
                10 + k, a3,
                lambda q, k=k, m3=m3: P3.at[k, m3, 0 : n2[k]],
                lambda q, k=k: P3.at[k, q, 0 : n2[k]],
            )
        )
    lax.fori_loop(cuts[1], cuts[2], pivot, 0)
    for k, (a1, a2, a3) in enumerate(orders):
        second[k]()
        row = base[k] + place[a1] * n1[k]
        spot = row + place[a2] * n2[k]
        low = slice(0, n2[k])
        out[pl.ds(spot, n2[k])] = P3[k, 0, low] + P3[k, 1, low] + P3[k, 2, low] + P3[k, 3, low]
        third.append(
            spread(
                13 + k, a2,
                lambda q, spot=spot, k=k: out.at[pl.ds(spot, n2[k])],
                lambda q, row=row, k=k: out.at[pl.ds(row + q * n2[k], n2[k])],
            )
        )
    lax.fori_loop(cuts[2], cuts[3], pivot, 0)
    for k, (a1, a2, a3) in enumerate(orders):
        third[k]()
        row = base[k] + place[a1] * n1[k]
        fourth.append(
            spread(
                16 + k, a1,
                lambda q, row=row, k=k: out.at[pl.ds(row, n1[k])],
                lambda q, k=k: out.at[pl.ds(base[k] + q * n1[k], n1[k])],
            )
        )
    lax.fori_loop(cuts[3], cuts[4], pivot, 0)
    m = M[...]
    diag = jnp.sum(jnp.where(lane_id == row_id, m, 0.0), axis=1, keepdims=True)
    linv = pltpu.roll(m / jnp.sqrt(diag), rank, 1)[:, 0:rank]
    ortho_out[...] = jnp.dot(linv, (L1[0] + L1[1] + L1[2] + L1[3]) * (1.0 / 8.0), precision=HI, preferred_element_type=f32)
    v_high, v_low = split(linv * (1.0 / 8.0))
    LV[0] = v_high
    LV[1] = v_low
    for k in range(3):
        fourth[k]()
        r = pl.ds(base[k], sizes[k])
        swap(20, out.at[r], out.at[r], k)

    def right(j, sq):
        high, low = split(jnp.concatenate([tile_column(out, 2 * j), tile_column(out, 2 * j + 1)], axis=1))
        v = dot(LV[0], high) + dot(LV[1], high) + dot(LV[0], low)
        RT[:, cols_of(j * 256, 256)] = v
        return sq + v * v

    sq = jnp.zeros((rank, 256), f32)
    sq_other = sq
    for k in range(3):
        sq = lax.fori_loop(*part_blocks(c, k), right, sq)
    for k in range(3):
        r = pl.ds(theirs + begin[k], sizes[k])
        remote(out.at[r], out.at[r], send.at[20, k], recv.at[20, k], mate).wait_recv()
        sq_other = lax.fori_loop(*part_blocks(1 - c, k), right, sq_other)
    total = jnp.where(c == 0, sq, sq_other) + jnp.where(c == 0, sq_other, sq)
    norm = lax.rsqrt(jnp.sum(total, axis=1, keepdims=True) + EPS)
    norm_out[...] = jnp.broadcast_to(norm, norm_out.shape)

    for copy in pending + sent:
        copy.wait_send()
    for by in (1, 2, 3):
        for xx in range(4):
            zz = around(pa, by)
            remote(codes.at[xx, zz], R.at[0, 0], sc.at[xx, zz], rc.at[0, 0], along("a", ar)).wait_send()
            remote(scales.at[xx, zz], RS.at[0, 0], ss.at[xx, zz], rs.at[0, 0], along("a", ar)).wait_send()
    for o in range(4):
        side, n = o % 2, o // 2
        remote(relay.at[side, n], R.at[0, 0], sf.at[side, n], rc.at[0, 0], along("a", ar)).wait_send()
        remote(relay_s.at[side, n], RS.at[0, 0], sfs.at[side, n], rs.at[0, 0], along("a", ar)).wait_send()


def communicate(cot, bt, lengths, mom, rft):
    tok, rows = cot.shape
    feats = bt.shape[0]
    rank, cols = rft.shape
    tiles = cols // 128 * (rank // 8)
    half = tiles // 2
    most = max(parts_of(half))
    n1, n2 = most // 4, most // 16
    return pl.pallas_call(
        comm_kernel,
        out_shape=(
            jax.ShapeDtypeStruct((rows, cols), f32),
            jax.ShapeDtypeStruct((rank, cols), f32),
            jax.ShapeDtypeStruct((rank, 128), f32),
            jax.ShapeDtypeStruct((rank, rows), f32),
        ),
        in_specs=[hspec(), hspec(), sspec(), hspec(), hspec()],
        out_specs=(vspec(), vspec(), vspec(), vspec()),
        scratch_shapes=[
            VMEM((4, tok, rows), bf16),
            VMEM((4, feats, tok), bf16),
            VMEM((4, 4, feats, rows), jnp.int16),
            VMEM((4, 4, 8, rows), f32),
            VMEM((4, 4, feats, rows), jnp.int16),
            VMEM((4, 4, 8, rows), f32),
            VMEM((2, 2, feats, rows), jnp.int16),
            VMEM((2, 2, 8, rows), f32),
            VMEM((feats, rows), f32),
            VMEM((16, tok), bf16),
            VMEM((2 * feats, rows), f32),
            VMEM((2 * rank, cols), bf16),
            VMEM((rank, cols), f32),
            VMEM((rank, rows), f32),
            VMEM((rank, rows), f32),
            VMEM((4, rank, rows), f32),
            VMEM((2 * rank, rows), bf16),
            VMEM((2, rank, rank), bf16),
            VMEM((tiles, 8, 128), f32),
            VMEM((half, 8, 128), f32),
            VMEM((tiles, 8, 128), f32),
            VMEM((3, 4, n1, 8, 128), f32),
            VMEM((3, 4, n2, 8, 128), f32),
            VMEM((3, 4, n2, 8, 128), f32),
            VMEM((4, rank, rank), f32),
            VMEM((4, rank, rank), f32),
            VMEM((rank, 2 * rank), f32),
            DMA((5,)), DMA((6,)), DMA((6,)), DMA((6,)), DMA((6,)),
            DMA((4, 4)), DMA((4, 4)), DMA((4, 4)), DMA((4, 4)),
            DMA((2, 2)), DMA((2, 2)), DMA((2, 2)), DMA((2, 2)),
            DMA((21, 4)), DMA((21, 4)),
        ],
        compiler_params=pltpu.CompilerParams(
            collective_id=0, has_side_effects=True, vmem_limit_bytes=COMM_BYTES
        ),
        name="communicate",
    )(cot, bt, lengths, mom, rft)


def finish_kernel(
    coef, right_t, norm, ortho_t, both, weight, new_weight, new_mom, new_right_t,
    bv, wv, NR, O3, osem,
):
    rows, cols = both.shape
    wide = cols // 8

    def store(i):
        r = cols_of(i * wide, wide)
        return (
            pltpu.make_async_copy(bv.at[:, r], new_mom.at[:, r], osem.at[i, 0]),
            pltpu.make_async_copy(wv.at[:, r], new_weight.at[:, r], osem.at[i, 1]),
            pltpu.make_async_copy(NR.at[:, r], new_right_t.at[:, r], osem.at[i, 2]),
        )

    both_t = jnp.concatenate([ortho_t[...] * (1.0 - MU), ortho_t[...] * (norm[:, 0:1] * coef)], axis=1)
    o_high, o_low = split(both_t)
    O3[...] = jnp.concatenate([o_high, o_high, o_low], axis=0).T

    def work(i, carry):
        r = cols_of(i * wide, wide)
        v = right_t[:, r]
        high, low = split(v)
        change = dot(O3[...], jnp.concatenate([high, low, high], axis=0))
        bv[:, r] = both[:, r] - change[0:rows]
        wv[:, r] = (weight[:, r].astype(f32) - change[rows:]).astype(bf16)
        NR[:, r] = v * norm[:, 0:1]
        for copy in store(i):
            copy.start()
        return carry

    lax.fori_loop(0, 8, work, 0)
    for i in range(8):
        for copy in store(i):
            copy.wait()


def finish(coef, right_t, norm, ortho_t, both, weight):
    rows, cols = both.shape
    rank = right_t.shape[0]
    return pl.pallas_call(
        functools.partial(finish_kernel, coef),
        out_shape=(
            jax.ShapeDtypeStruct((rows, cols), bf16),
            jax.ShapeDtypeStruct((rows, cols), f32),
            jax.ShapeDtypeStruct((rank, cols), f32),
        ),
        in_specs=[vspec()] * 5,
        out_specs=(hspec(), hspec(), hspec()),
        scratch_shapes=[
            VMEM((rows, cols), f32),
            VMEM((rows, cols), bf16),
            VMEM((rank, cols), f32),
            VMEM((2 * rows, 3 * rank), bf16),
            DMA((8, 3)),
        ],
        compiler_params=pltpu.CompilerParams(vmem_limit_bytes=FINISH_BYTES),
        name="finish",
    )(right_t, norm, ortho_t, both, weight)


def per_device(inputs, cotangent, lengths, momentum, weight, right_factor):
    stay = lambda v: pltpu.with_memory_space_constraint(v, pltpu.HBM)
    both, right_t, norm, ortho_t = communicate(
        stay(cotangent), stay(inputs.T), stay(lengths), stay(momentum[0]), stay(right_factor.T)
    )
    rows_all = both.shape[0] * lax.axis_size("tensor")
    coef = LR * math.sqrt(rows_all / both.shape[1])
    new_weight, new_mom, new_right_t = finish(coef, right_t, norm, ortho_t, both, weight)
    return (new_weight, new_mom[None], new_right_t.T)


def solution(mesh):
    placed = (
        P("dp", "tensor"),
        P("dp", "tensor"),
        P("dp"),
        P("dp", "tensor", None),
        P("tensor", None),
        P(),
    )
    return jax.shard_map(
        per_device,
        mesh=mesh,
        in_specs=placed,
        out_specs=(P("tensor", None), P("dp", "tensor", None), P()),
        check_vma=False,
    )
```

```python
import functools
import math

import jax
import jax.numpy as jnp
from jax import lax
from jax.experimental import pallas as pl
from jax.experimental.pallas import tpu as pltpu
from jax.sharding import PartitionSpec as P

EPS = 1e-06
MU = 0.95
LR = 0.02

f32 = jnp.float32
bf16 = jnp.bfloat16
HI = lax.Precision.HIGHEST
VMEM = pltpu.VMEM
DMA = pltpu.SemaphoreType.DMA
CODES = 32767.0
COMM_BYTES = 38 * 2**20
FINISH_BYTES = 16 * 2**20
DEPTH = 768


def vspec():
    return pl.BlockSpec(memory_space=pltpu.VMEM)


def hspec():
    return pl.BlockSpec(memory_space=pltpu.HBM)


def sspec():
    return pl.BlockSpec(memory_space=pltpu.SMEM)


def around(i, by):
    return lax.rem(i + by, 4)


def cols_of(start, size):
    return pl.ds(pl.multiple_of(start, 128), size)


def split(v):
    high = v.astype(bf16)
    return high, (v - high.astype(f32)).astype(bf16)


def dot(a, b, contract=((1,), (0,))):
    return lax.dot_general(a, b, (contract, ((), ())), preferred_element_type=f32)


def remote(src, dst, send, recv, where):
    return pltpu.make_async_remote_copy(
        src_ref=src,
        dst_ref=dst,
        send_sem=send,
        recv_sem=recv,
        device_id=where,
        device_id_type=pl.DeviceIdType.MESH,
    )


def greet(peers):
    barrier = pltpu.get_barrier_semaphore()
    for peer in peers:
        pl.semaphore_signal(barrier, inc=1, device_id=peer, device_id_type=pl.DeviceIdType.MESH)
    pl.semaphore_wait(barrier, len(peers))


def parts_of(tiles):
    most = tiles // 16 - 2 * (tiles // 48)
    return (most * 16, tiles // 48 * 16, tiles // 48 * 16)


def tile_column(tiles, j):
    return tiles[pl.ds(j * 8, 8)].reshape(64, 128)


def comm_kernel(
    cot, bt, lengths, mom, rft, both, RT, norm_out, ortho_out,
    A, B, codes, scales, R, RS, relay, relay_s, acc, keep, S, R2, rfv,
    LT, L0, L1, LF, LL, LV, T, D, out, P1, P2, P3, G1, G2, M,
    sl, sa, ra, sb, rb, sc, ss, rc, rs, sf, sfs, rf, rfs, send, recv,
):
    t = lax.axis_index("tensor")
    d = lax.axis_index("dp")
    x, z = lax.div(t, 4), lax.rem(t, 4)
    y, c = lax.div(d, 2), lax.rem(d, 2)
    place = {"x": x, "y": y, "z": z}

    def along(axis, k):
        if axis == "core":
            return {"dp": y * 2 + k}
        if axis == "y":
            return {"dp": k * 2 + c}
        if axis == "x":
            return {"tensor": k * 4 + z}
        if axis == "z":
            return {"tensor": x * 4 + k}
        if axis == "a":
            return {"tensor": (1 - c) * (x * 4 + k) + c * (k * 4 + z)}
        return {"tensor": (1 - c) * (k * 4 + z) + c * (x * 4 + k)}

    pa = (1 - c) * z + c * x
    pb = (1 - c) * x + c * z
    al, ar, ao = around(pa, 3), around(pa, 1), around(pa, 2)
    bl, br, bo = around(pb, 3), around(pb, 1), around(pb, 2)
    tok, rows = cot.shape
    feats = bt.shape[0]
    ha, hb = tok // 2, feats // 2
    mate = along("core", 1 - c)

    locals_ = [
        pltpu.make_async_copy(cot, A.at[pa], sl.at[0]),
        pltpu.make_async_copy(bt, B.at[pb], sl.at[1]),
        pltpu.make_async_copy(mom, both, sl.at[2]),
        pltpu.make_async_copy(rft, rfv, sl.at[3]),
    ]
    greet([mate] + [along(a, around(place[a], q)) for a in "xyz" for q in (1, 2, 3)])

    def part_a(h):
        return pl.ds(h * ha, ha)

    def part_b(h):
        return pl.ds(h * hb, hb)

    sent = []
    for half, right in ((0, True), (1, False), (1, True), (0, False)):
        k = half + (0 if right else 2)
        ca = remote(cot.at[part_a(half)], A.at[pa, part_a(half)], sa.at[k], ra.at[k], along("a", ar if right else al))
        ca.start()
        cb = remote(bt.at[part_b(half)], B.at[pb, part_b(half)], sb.at[k], rb.at[k], along("b", br if right else bl))
        cb.start()
        sent += [ca, cb]
    for copy in locals_:
        copy.start()

    def got_a(k):
        remote(A.at[pa, part_a(0)], A.at[pa, part_a(0)], sa.at[0], ra.at[k], along("a", ar)).wait_recv()

    def got_b(k):
        remote(B.at[pb, part_b(0)], B.at[pb, part_b(0)], sb.at[0], rb.at[k], along("b", br)).wait_recv()

    def pass_a(k, half, origin, to):
        copy = remote(A.at[origin, part_a(half)], A.at[origin, part_a(half)], sa.at[k], ra.at[k], along("a", to))
        copy.start()
        sent.append(copy)

    def pass_b(k, half, origin, to):
        copy = remote(B.at[origin, part_b(half)], B.at[origin, part_b(half)], sb.at[k], rb.at[k], along("b", to))
        copy.start()
        sent.append(copy)

    block_len = tok // lengths.shape[0]
    count = lengths[0]
    for b in range(lengths.shape[0]):
        keep[:, b * block_len : (b + 1) * block_len] = (
            lax.broadcasted_iota(jnp.int32, (16, block_len), 1) < lengths[b]
        ).astype(f32).astype(bf16)
        if b:
            count = count + lengths[b]
    share = 1.0 / jnp.full((1, rows), count, jnp.int32).astype(f32)

    def unit(xx, zz, code_ref, scale_ref):
        acc[...] = jnp.zeros_like(acc)

        def step(k, carry):
            r = cols_of(k * DEPTH, DEPTH)
            acc[...] += dot(B[xx, :, r] * keep[0:1, r], A[zz, r, :])
            return carry

        lax.fori_loop(0, tok // DEPTH, step, 0)
        v = acc[...] * share
        top = jnp.max(jnp.abs(v), axis=0, keepdims=True)
        live = top > 1e-30
        code = jnp.round(v * jnp.where(live, CODES / jnp.where(live, top, 1.0), 0.0))
        code_ref[...] = code.astype(jnp.int32).astype(jnp.int16)
        scale_ref[...] = jnp.broadcast_to(jnp.where(live, top, 0.0) * (1.0 / CODES), (8, rows))

    def made(xx, zz):
        unit(xx, zz, codes.at[xx, zz], scales.at[xx, zz])

    def home(xx, zz):
        remote(codes.at[xx, zz], R.at[xx, pa], sc.at[xx, zz], rc.at[xx, pa], along("a", zz)).start()
        remote(scales.at[xx, zz], RS.at[xx, pa], ss.at[xx, zz], rs.at[xx, pa], along("a", zz)).start()

    def half_way(xx, side, n):
        to = along("a", around(pa, jnp.where(side == 0, 1, 3)))
        remote(codes.at[xx, ao], relay.at[side, n], sc.at[xx, ao], rf.at[side, n], to).start()
        remote(scales.at[xx, ao], relay_s.at[side, n], ss.at[xx, ao], rfs.at[side, n], to).start()

    def hand_on(o, wait_only=False):
        side, n = o % 2, o // 2
        xx = (pb, bl, br, bo)[o]
        origin, to = (al, ar) if side == 0 else (ar, al)
        one = remote(relay.at[side, n], R.at[xx, origin], sf.at[side, n], rf.at[side, n], along("a", to))
        one.wait_recv()
        two = remote(relay_s.at[side, n], RS.at[xx, origin], sfs.at[side, n], rfs.at[side, n], along("a", to))
        two.wait_recv()
        remote(relay.at[side, n], R.at[xx, origin], sf.at[side, n], rc.at[xx, origin], along("a", to)).start()
        remote(relay_s.at[side, n], RS.at[xx, origin], sfs.at[side, n], rs.at[xx, origin], along("a", to)).start()

    locals_[0].wait()
    locals_[1].wait()
    unit(pb, pa, R.at[pb, pa], RS.at[pb, pa])
    locals_[2].wait()
    locals_[3].wait()
    rank = rft.shape[0]
    r_high, r_low = split(rfv[...])
    R2[0:rank] = r_high
    R2[rank : 2 * rank] = r_low
    LT[...] = jnp.zeros_like(LT)

    def mom_left(g, carry):
        r = cols_of(g * 256, 256)
        high, low = split(both[:, r])
        v = dot(R2[:, r], high, ((1,), (1,)))
        LT[...] += v[0:rank] + v[rank:] + dot(R2[0:rank, r], low, ((1,), (1,)))
        return carry

    lax.fori_loop(0, both.shape[1] // 256, mom_left, 0)

    got_a(0)
    pass_a(4, 0, al, ar)
    got_a(3)
    pass_a(5, 1, ar, al)
    got_b(0)
    pass_b(4, 0, bl, br)
    got_b(3)
    pass_b(5, 1, br, bl)
    got_a(1)
    got_a(2)

    def own_cols(i, carry):
        zz = around(pa, 3 - 2 * i)
        made(pb, zz)
        home(pb, zz)
        return carry

    lax.fori_loop(0, 2, own_cols, 0)
    got_b(1)
    got_b(2)

    def next_cols(i, carry):
        xx = around(pb, 3 - 2 * lax.div(i, 3))
        m = lax.rem(i, 3)

        @pl.when(m == 2)
        def _():
            unit(xx, pa, R.at[xx, pa], RS.at[xx, pa])

        @pl.when(m != 2)
        def _():
            made(xx, around(pa, 3 - 2 * m))

        return carry

    lax.fori_loop(0, 6, next_cols, 0)
    got_a(4)
    got_a(5)

    def far_rows(i, carry):
        xx = around(pb, jnp.where(i == 0, 0, 5 - 2 * i))
        made(xx, ao)
        half_way(xx, lax.rem(i, 2), lax.div(i, 2))
        return carry

    lax.fori_loop(0, 3, far_rows, 0)
    for xx in (bl, br):
        home(xx, al)
        home(xx, ar)
    for o in range(3):
        hand_on(o)
    got_b(4)
    got_b(5)

    def far_cols(i, carry):
        @pl.when(i == 0)
        def _():
            made(bo, ao)
            half_way(bo, 1, 1)

        @pl.when(jnp.logical_and(i != 0, i != 3))
        def _():
            zz = around(pa, 5 - 2 * i)
            made(bo, zz)
            home(bo, zz)

        @pl.when(i == 3)
        def _():
            unit(bo, pa, R.at[bo, pa], RS.at[bo, pa])

        return carry

    lax.fori_loop(0, 4, far_cols, 0)
    late, far = lax.div(bo, 2), lax.div(ao, 2)

    def gather_home(n, carry):
        o = jnp.where(n < 6, lax.rem(n, 3), 3)
        h = jnp.where(jnp.logical_or(n < 3, n == 6), 1 - far, far)
        xx = around(pb, jnp.where(o == 0, 0, jnp.where(o == 3, 2, 5 - 2 * o)))
        group = jnp.where(n < 4, 1 - late, late)
        m = lax.rem(n, 4)
        zz = around(pa, jnp.where(m == 0, 0, jnp.where(m == 3, 2, 5 - 2 * m)))
        base = jnp.where(c == 0, xx * 2 + h, zz * 2 + group) * (2 * feats)
        for i in range(2):
            xi = jnp.where(c == 0, xx, 2 * group + i)
            zi = jnp.where(c == 0, 2 * h + i, zz)

            @pl.when(zi != pa)
            def _():
                remote(codes.at[0, 0], R.at[xi, zi], sc.at[0, 0], rc.at[xi, zi], along("a", ar)).wait_recv()
                remote(scales.at[0, 0], RS.at[xi, zi], ss.at[0, 0], rs.at[xi, zi], along("a", ar)).wait_recv()

            S[i * feats : (i + 1) * feats] = R[xi, zi].astype(jnp.int32).astype(f32) * RS[xi, zi, 0:1]
        high, low = split(S[...])
        r = cols_of(base, 2 * feats)
        v = dot(R2[:, r], high)
        LT[...] += v[0:rank] + v[rank:] + dot(R2[0:rank, r], low)
        for i in range(2 * feats // 128):
            both[:, cols_of(base + 128 * i, 128)] += S[128 * i : 128 * (i + 1)].T
        return carry

    lax.fori_loop(0, 3, gather_home, 0)
    hand_on(3)
    lax.fori_loop(3, 8, gather_home, 0)

    pending = []

    def swap(stage, src, dst, k=0):
        copy = remote(src, dst, send.at[stage, k], recv.at[stage, k], mate)
        copy.start()
        pending.append(copy)
        return copy

    def spread(stage, axis, src, dst):
        me = place[axis]
        waits = {}
        for q in (2, 1, 3):
            k = around(me, q)
            copy = remote(src(k), dst(me), send.at[stage, q], recv.at[stage, q], along(axis, k))
            copy.start()
            pending.append(copy)
            waits[q] = remote(src(k), dst(around(me, 4 - q)), send.at[stage, q], recv.at[stage, q], along(axis, k))

        def wait(which=(2, 1, 3)):
            for q in which:
                waits[q].wait_recv()

        return wait

    here, there = pl.ds(c * (rank // 2), rank // 2), pl.ds((1 - c) * (rank // 2), rank // 2)
    swap(0, LT.at[there], L0).wait_recv()
    L1[y] = LT[here] + L0[...]
    spread(1, "y", lambda k: L1.at[y], lambda k: L1.at[k])()
    LF[here] = (L1[0] + L1[1] + L1[2] + L1[3]) * (1.0 / 8.0)
    swap(2, LF.at[here], LF.at[here])
    remote(LF.at[there], LF.at[there], send.at[2, 0], recv.at[2, 0], mate).wait_recv()
    left = LF[...]
    left_high, left_low = split(left)
    LL[0:rank] = left_high
    LL[rank : 2 * rank] = left_low
    v = dot(LL[...], left_high, ((1,), (1,)))
    G1[z] = v[0:rank] + v[rank:] + dot(left_high, left_low, ((1,), (1,)))
    gram_wait = spread(21, "z", lambda k: G1.at[z], lambda k: G1.at[k])

    tiles = both.shape[1] // 128 * (rank // 8)
    half = tiles // 2
    blocks = both.shape[1] // 512

    def block(g, carry):
        high, low = split(both[:, cols_of(g * 256, 256)])
        v = dot(LL[...], high)
        v = v[0:rank] + v[rank:] + dot(LL[0:rank], low)
        for i in range(2):
            T[pl.ds(g * 16 + i * 8, 8)] = v[:, 128 * i : 128 * (i + 1)].reshape(8, 8, 128)
        return carry

    orders = (("y", "x", "z"), ("x", "z", "y"), ("z", "y", "x"))
    sizes = parts_of(half)
    begin = (0, sizes[0], sizes[0] + sizes[1])
    mine, theirs = c * half, (1 - c) * half
    base = [mine + start for start in begin]
    n1 = [size // 4 for size in sizes]
    n2 = [size // 16 for size in sizes]

    def part_blocks(side, k):
        start = blocks * side + begin[k] // 16
        return start, start + sizes[k] // 16

    core_waits = []
    for k in range(3):
        lax.fori_loop(*part_blocks(1 - c, k), block, 0)
        core_waits.append(
            swap(3, T.at[pl.ds(theirs + begin[k], sizes[k])], D.at[pl.ds(begin[k], sizes[k])], k)
        )

    def add_core(g, carry):
        r = pl.ds(mine + g * 16, 16)
        T[r] = T[r] + D[pl.ds(g * 16, 16)]
        return carry

    zeroth, first, second, third = [], [], [], []
    for k, (a1, a2, a3) in enumerate(orders):
        lax.fori_loop(*part_blocks(c, k), block, 0)
        core_waits[k].wait_recv()
        lax.fori_loop(begin[k] // 16, (begin[k] + sizes[k]) // 16, add_core, 0)
        zeroth.append(
            spread(
                4 + k, a1,
                lambda q, k=k: T.at[pl.ds(base[k] + q * n1[k], n1[k])],
                lambda q, k=k: P1.at[k, q, 0 : n1[k]],
            )
        )
    gram_wait()
    G2[x] = G1[0] + G1[1] + G1[2] + G1[3]
    gram_wait = spread(19, "x", lambda k: G2.at[x], lambda k: G2.at[k])
    for k, (a1, a2, a3) in enumerate(orders):
        me = place[a1]
        P1[k, me, 0 : n1[k]] = T[pl.ds(base[k] + me * n1[k], n1[k])]
        zeroth[k]()
        low = slice(0, n1[k])
        P1[k, 0, low] = P1[k, 0, low] + P1[k, 1, low] + P1[k, 2, low] + P1[k, 3, low]
        first.append(
            spread(
                7 + k, a2,
                lambda q, k=k: P1.at[k, 0, pl.ds(q * n2[k], n2[k])],
                lambda q, k=k: P2.at[k, q, 0 : n2[k]],
            )
        )
    row_id = lax.broadcasted_iota(jnp.int32, (rank, 2 * rank), 0)
    lane_id = lax.broadcasted_iota(jnp.int32, (rank, 2 * rank), 1)
    gram_wait()
    M[...] = jnp.where(lane_id == row_id + rank, 1.0, 0.0)
    M[:, 0:rank] = G2[0] + G2[1] + G2[2] + G2[3]

    def pivot(k, carry):
        m = M[...]
        row = M[pl.ds(k, 1), :]
        top = jnp.sum(jnp.where(lane_id[0:1] == k, row, 0.0), axis=1, keepdims=True)
        factor = jnp.sum(jnp.where(lane_id == k, m, 0.0), axis=1, keepdims=True)
        factor = jnp.where(row_id[:, 0:1] > k, factor / top, 0.0)
        M[...] = m - factor * row
        return carry

    cuts = (0, 16, 32, 48, rank)
    lax.fori_loop(cuts[0], cuts[1], pivot, 0)
    for k, (a1, a2, a3) in enumerate(orders):
        me = place[a2]
        low = slice(0, n2[k])
        P2[k, me, low] = P1[k, 0, pl.ds(me * n2[k], n2[k])]
        first[k]()
        m3 = place[a3]
        P3[k, m3, low] = P2[k, 0, low] + P2[k, 1, low] + P2[k, 2, low] + P2[k, 3, low]
        second.append(
            spread(
                10 + k, a3,
                lambda q, k=k, m3=m3: P3.at[k, m3, 0 : n2[k]],
                lambda q, k=k: P3.at[k, q, 0 : n2[k]],
            )
        )
    lax.fori_loop(cuts[1], cuts[2], pivot, 0)
    for k, (a1, a2, a3) in enumerate(orders):
        second[k]()
        row = base[k] + place[a1] * n1[k]
        spot = row + place[a2] * n2[k]
        low = slice(0, n2[k])
        out[pl.ds(spot, n2[k])] = P3[k, 0, low] + P3[k, 1, low] + P3[k, 2, low] + P3[k, 3, low]
        third.append(
            spread(
                13 + k, a2,
                lambda q, spot=spot, k=k: out.at[pl.ds(spot, n2[k])],
                lambda q, row=row, k=k: out.at[pl.ds(row + q * n2[k], n2[k])],
            )
        )
    def last(k, n):
        a1, a2, a3 = orders[k]
        spot = around(place[a2], 4 - n) * n2[k]
        fourth[k].append(
            spread(
                22 + 4 * k + n, a1,
                lambda q: out.at[pl.ds(base[k] + place[a1] * n1[k] + spot, n2[k])],
                lambda q: out.at[pl.ds(base[k] + q * n1[k] + spot, n2[k])],
            )
        )

    fourth = [[], [], []]
    for k in range(3):
        last(k, 0)
    lax.fori_loop(cuts[2], cuts[3], pivot, 0)
    for n in (1, 3, 2):
        for k in range(3):
            third[k]((n,))
            last(k, n)
    lax.fori_loop(cuts[3], cuts[4], pivot, 0)
    m = M[...]
    diag = jnp.sum(jnp.where(lane_id == row_id, m, 0.0), axis=1, keepdims=True)
    linv = pltpu.roll(m / jnp.sqrt(diag), rank, 1)[:, 0:rank]
    ortho_out[...] = jnp.dot(linv, LF[...], precision=HI, preferred_element_type=f32)
    v_high, v_low = split(linv * (1.0 / 8.0))
    LV[0] = v_high
    LV[1] = v_low
    for k in range(3):
        for done in fourth[k]:
            done()
        r = pl.ds(base[k], sizes[k])
        swap(20, out.at[r], out.at[r], k)

    def right(j, sq):
        high, low = split(jnp.concatenate([tile_column(out, 2 * j), tile_column(out, 2 * j + 1)], axis=1))
        v = dot(LV[0], high) + dot(LV[1], high) + dot(LV[0], low)
        RT[:, cols_of(j * 256, 256)] = v
        return sq + v * v

    sq = jnp.zeros((rank, 256), f32)
    sq_other = sq
    for k in range(3):
        sq = lax.fori_loop(*part_blocks(c, k), right, sq)
    for k in range(3):
        r = pl.ds(theirs + begin[k], sizes[k])
        remote(out.at[r], out.at[r], send.at[20, k], recv.at[20, k], mate).wait_recv()
        sq_other = lax.fori_loop(*part_blocks(1 - c, k), right, sq_other)
    total = jnp.where(c == 0, sq, sq_other) + jnp.where(c == 0, sq_other, sq)
    norm = lax.rsqrt(jnp.sum(total, axis=1, keepdims=True) + EPS)
    norm_out[...] = jnp.broadcast_to(norm, norm_out.shape)

    for copy in pending + sent:
        copy.wait_send()
    for by in (1, 2, 3):
        for xx in range(4):
            zz = around(pa, by)
            remote(codes.at[xx, zz], R.at[0, 0], sc.at[xx, zz], rc.at[0, 0], along("a", ar)).wait_send()
            remote(scales.at[xx, zz], RS.at[0, 0], ss.at[xx, zz], rs.at[0, 0], along("a", ar)).wait_send()
    for o in range(4):
        side, n = o % 2, o // 2
        remote(relay.at[side, n], R.at[0, 0], sf.at[side, n], rc.at[0, 0], along("a", ar)).wait_send()
        remote(relay_s.at[side, n], RS.at[0, 0], sfs.at[side, n], rs.at[0, 0], along("a", ar)).wait_send()


def communicate(cot, bt, lengths, mom, rft):
    tok, rows = cot.shape
    feats = bt.shape[0]
    rank, cols = rft.shape
    tiles = cols // 128 * (rank // 8)
    half = tiles // 2
    most = max(parts_of(half))
    n1, n2 = most // 4, most // 16
    return pl.pallas_call(
        comm_kernel,
        out_shape=(
            jax.ShapeDtypeStruct((rows, cols), f32),
            jax.ShapeDtypeStruct((rank, cols), f32),
            jax.ShapeDtypeStruct((rank, 128), f32),
            jax.ShapeDtypeStruct((rank, rows), f32),
        ),
        in_specs=[hspec(), hspec(), sspec(), hspec(), hspec()],
        out_specs=(vspec(), vspec(), vspec(), vspec()),
        scratch_shapes=[
            VMEM((4, tok, rows), bf16),
            VMEM((4, feats, tok), bf16),
            VMEM((4, 4, feats, rows), jnp.int16),
            VMEM((4, 4, 8, rows), f32),
            VMEM((4, 4, feats, rows), jnp.int16),
            VMEM((4, 4, 8, rows), f32),
            VMEM((2, 2, feats, rows), jnp.int16),
            VMEM((2, 2, 8, rows), f32),
            VMEM((feats, rows), f32),
            VMEM((16, tok), bf16),
            VMEM((2 * feats, rows), f32),
            VMEM((2 * rank, cols), bf16),
            VMEM((rank, cols), f32),
            VMEM((rank, rows), f32),
            VMEM((rank // 2, rows), f32),
            VMEM((4, rank // 2, rows), f32),
            VMEM((rank, rows), f32),
            VMEM((2 * rank, rows), bf16),
            VMEM((2, rank, rank), bf16),
            VMEM((tiles, 8, 128), f32),
            VMEM((half, 8, 128), f32),
            VMEM((tiles, 8, 128), f32),
            VMEM((3, 4, n1, 8, 128), f32),
            VMEM((3, 4, n2, 8, 128), f32),
            VMEM((3, 4, n2, 8, 128), f32),
            VMEM((4, rank, rank), f32),
            VMEM((4, rank, rank), f32),
            VMEM((rank, 2 * rank), f32),
            DMA((5,)), DMA((6,)), DMA((6,)), DMA((6,)), DMA((6,)),
            DMA((4, 4)), DMA((4, 4)), DMA((4, 4)), DMA((4, 4)),
            DMA((2, 2)), DMA((2, 2)), DMA((2, 2)), DMA((2, 2)),
            DMA((34, 4)), DMA((34, 4)),
        ],
        compiler_params=pltpu.CompilerParams(
            collective_id=0, has_side_effects=True, vmem_limit_bytes=COMM_BYTES
        ),
        name="communicate",
    )(cot, bt, lengths, mom, rft)


def finish_kernel(
    coef, right_t, norm, ortho_t, both, weight, new_weight, new_mom, new_right_t,
    bv, wv, NR, O3, osem,
):
    rows, cols = both.shape
    wide = cols // 8

    def store(i):
        r = cols_of(i * wide, wide)
        return (
            pltpu.make_async_copy(bv.at[:, r], new_mom.at[:, r], osem.at[i, 0]),
            pltpu.make_async_copy(wv.at[:, r], new_weight.at[:, r], osem.at[i, 1]),
            pltpu.make_async_copy(NR.at[:, r], new_right_t.at[:, r], osem.at[i, 2]),
        )

    both_t = jnp.concatenate([ortho_t[...] * (1.0 - MU), ortho_t[...] * (norm[:, 0:1] * coef)], axis=1)
    o_high, o_low = split(both_t)
    O3[...] = jnp.concatenate([o_high, o_high, o_low], axis=0).T

    def work(i, carry):
        r = cols_of(i * wide, wide)
        v = right_t[:, r]
        high, low = split(v)
        change = dot(O3[...], jnp.concatenate([high, low, high], axis=0))
        bv[:, r] = both[:, r] - change[0:rows]
        wv[:, r] = (weight[:, r].astype(f32) - change[rows:]).astype(bf16)
        NR[:, r] = v * norm[:, 0:1]
        for copy in store(i):
            copy.start()
        return carry

    lax.fori_loop(0, 8, work, 0)
    for i in range(8):
        for copy in store(i):
            copy.wait()


def finish(coef, right_t, norm, ortho_t, both, weight):
    rows, cols = both.shape
    rank = right_t.shape[0]
    return pl.pallas_call(
        functools.partial(finish_kernel, coef),
        out_shape=(
            jax.ShapeDtypeStruct((rows, cols), bf16),
            jax.ShapeDtypeStruct((rows, cols), f32),
            jax.ShapeDtypeStruct((rank, cols), f32),
        ),
        in_specs=[vspec()] * 5,
        out_specs=(hspec(), hspec(), hspec()),
        scratch_shapes=[
            VMEM((rows, cols), f32),
            VMEM((rows, cols), bf16),
            VMEM((rank, cols), f32),
            VMEM((2 * rows, 3 * rank), bf16),
            DMA((8, 3)),
        ],
        compiler_params=pltpu.CompilerParams(vmem_limit_bytes=FINISH_BYTES),
        name="finish",
    )(right_t, norm, ortho_t, both, weight)


def per_device(inputs, cotangent, lengths, momentum, weight, right_factor):
    stay = lambda v: pltpu.with_memory_space_constraint(v, pltpu.HBM)
    both, right_t, norm, ortho_t = communicate(
        stay(cotangent), stay(inputs.T), stay(lengths), stay(momentum[0]), stay(right_factor.T)
    )
    rows_all = both.shape[0] * lax.axis_size("tensor")
    coef = LR * math.sqrt(rows_all / both.shape[1])
    new_weight, new_mom, new_right_t = finish(coef, right_t, norm, ortho_t, both, weight)
    return (new_weight, new_mom[None], new_right_t.T)


def solution(mesh):
    placed = (
        P("dp", "tensor"),
        P("dp", "tensor"),
        P("dp"),
        P("dp", "tensor", None),
        P("tensor", None),
        P(),
    )
    return jax.shard_map(
        per_device,
        mesh=mesh,
        in_specs=placed,
        out_specs=(P("tensor", None), P("dp", "tensor", None), P()),
        check_vma=False,
    )
```

```python
import functools
import math

import jax
import jax.numpy as jnp
from jax import lax
from jax.experimental import pallas as pl
from jax.experimental.pallas import tpu as pltpu
from jax.sharding import PartitionSpec as P

EPS = 1e-06
MU = 0.95
LR = 0.02

f32 = jnp.float32
bf16 = jnp.bfloat16
HI = lax.Precision.HIGHEST
VMEM = pltpu.VMEM
DMA = pltpu.SemaphoreType.DMA
CODES = 32767.0
COMM_BYTES = 38 * 2**20
FINISH_BYTES = 16 * 2**20
DEPTH = 1536


def vspec():
    return pl.BlockSpec(memory_space=pltpu.VMEM)


def hspec():
    return pl.BlockSpec(memory_space=pltpu.HBM)


def sspec():
    return pl.BlockSpec(memory_space=pltpu.SMEM)


def around(i, by):
    return lax.rem(i + by, 4)


def cols_of(start, size):
    return pl.ds(pl.multiple_of(start, 128), size)


def split(v):
    high = v.astype(bf16)
    return high, (v - high.astype(f32)).astype(bf16)


def dot(a, b, contract=((1,), (0,))):
    return lax.dot_general(a, b, (contract, ((), ())), preferred_element_type=f32)


def remote(src, dst, send, recv, where):
    return pltpu.make_async_remote_copy(
        src_ref=src,
        dst_ref=dst,
        send_sem=send,
        recv_sem=recv,
        device_id=where,
        device_id_type=pl.DeviceIdType.MESH,
    )


def greet(peers):
    barrier = pltpu.get_barrier_semaphore()
    for peer in peers:
        pl.semaphore_signal(barrier, inc=1, device_id=peer, device_id_type=pl.DeviceIdType.MESH)
    pl.semaphore_wait(barrier, len(peers))


def parts_of(tiles):
    most = tiles // 16 - 2 * (tiles // 48)
    return (most * 16, tiles // 48 * 16, tiles // 48 * 16)


def tile_column(tiles, j):
    return tiles[pl.ds(j * 8, 8)].reshape(64, 128)


def comm_kernel(
    cot, bt, lengths, mom, rft, both, RT, norm_out, ortho_out,
    A, B, codes, scales, R, RS, relay, relay_s, acc, keep, S, R2, rfv,
    LT, L0, L1, LL, LV, T, D, out, P1, P2, P3, G1, G2, M,
    sl, sa, ra, sb, rb, sc, ss, rc, rs, sf, sfs, rf, rfs, send, recv,
):
    t = lax.axis_index("tensor")
    d = lax.axis_index("dp")
    x, z = lax.div(t, 4), lax.rem(t, 4)
    y, c = lax.div(d, 2), lax.rem(d, 2)
    place = {"x": x, "y": y, "z": z}

    def along(axis, k):
        if axis == "core":
            return {"dp": y * 2 + k}
        if axis == "y":
            return {"dp": k * 2 + c}
        if axis == "x":
            return {"tensor": k * 4 + z}
        if axis == "z":
            return {"tensor": x * 4 + k}
        if axis == "a":
            return {"tensor": (1 - c) * (x * 4 + k) + c * (k * 4 + z)}
        return {"tensor": (1 - c) * (k * 4 + z) + c * (x * 4 + k)}

    pa = (1 - c) * z + c * x
    pb = (1 - c) * x + c * z
    al, ar, ao = around(pa, 3), around(pa, 1), around(pa, 2)
    bl, br, bo = around(pb, 3), around(pb, 1), around(pb, 2)
    tok, rows = cot.shape
    feats = bt.shape[0]
    ha, hb = tok // 2, feats // 2
    mate = along("core", 1 - c)

    locals_ = [
        pltpu.make_async_copy(cot, A.at[pa], sl.at[0]),
        pltpu.make_async_copy(bt, B.at[pb], sl.at[1]),
        pltpu.make_async_copy(mom, both, sl.at[2]),
        pltpu.make_async_copy(rft, rfv, sl.at[3]),
    ]
    for copy in locals_:
        copy.start()
    greet([mate] + [along(a, around(place[a], q)) for a in "xyz" for q in (1, 2, 3)])

    def part_a(h):
        return pl.ds(h * ha, ha)

    def part_b(h):
        return pl.ds(h * hb, hb)

    sent = []
    for half, right in ((0, True), (1, False), (1, True), (0, False)):
        k = half + (0 if right else 2)
        ca = remote(cot.at[part_a(half)], A.at[pa, part_a(half)], sa.at[k], ra.at[k], along("a", ar if right else al))
        ca.start()
        cb = remote(bt.at[part_b(half)], B.at[pb, part_b(half)], sb.at[k], rb.at[k], along("b", br if right else bl))
        cb.start()
        sent += [ca, cb]

    def got_a(k):
        remote(A.at[pa, part_a(0)], A.at[pa, part_a(0)], sa.at[0], ra.at[k], along("a", ar)).wait_recv()

    def got_b(k):
        remote(B.at[pb, part_b(0)], B.at[pb, part_b(0)], sb.at[0], rb.at[k], along("b", br)).wait_recv()

    def pass_a(k, half, origin, to):
        copy = remote(A.at[origin, part_a(half)], A.at[origin, part_a(half)], sa.at[k], ra.at[k], along("a", to))
        copy.start()
        sent.append(copy)

    def pass_b(k, half, origin, to):
        copy = remote(B.at[origin, part_b(half)], B.at[origin, part_b(half)], sb.at[k], rb.at[k], along("b", to))
        copy.start()
        sent.append(copy)

    block_len = tok // lengths.shape[0]
    count = lengths[0]
    for b in range(lengths.shape[0]):
        keep[:, b * block_len : (b + 1) * block_len] = (
            lax.broadcasted_iota(jnp.int32, (16, block_len), 1) < lengths[b]
        ).astype(f32).astype(bf16)
        if b:
            count = count + lengths[b]
    share = 1.0 / jnp.full((1, rows), count, jnp.int32).astype(f32)

    def unit(xx, zz, code_ref, scale_ref):
        acc[...] = jnp.zeros_like(acc)

        def step(k, carry):
            r = cols_of(k * DEPTH, DEPTH)
            acc[...] += dot(B[xx, :, r] * keep[0:1, r], A[zz, r, :])
            return carry

        lax.fori_loop(0, tok // DEPTH, step, 0)
        v = acc[...] * share
        top = jnp.max(jnp.abs(v), axis=0, keepdims=True)
        live = top > 1e-30
        code = jnp.round(v * jnp.where(live, CODES / jnp.where(live, top, 1.0), 0.0))
        code_ref[...] = code.astype(jnp.int32).astype(jnp.int16)
        scale_ref[...] = jnp.broadcast_to(jnp.where(live, top, 0.0) * (1.0 / CODES), (8, rows))

    def made(xx, zz):
        unit(xx, zz, codes.at[xx, zz], scales.at[xx, zz])

    def home(xx, zz):
        remote(codes.at[xx, zz], R.at[xx, pa], sc.at[xx, zz], rc.at[xx, pa], along("a", zz)).start()
        remote(scales.at[xx, zz], RS.at[xx, pa], ss.at[xx, zz], rs.at[xx, pa], along("a", zz)).start()

    def half_way(xx, side, n):
        to = along("a", around(pa, jnp.where(side == 0, 1, 3)))
        remote(codes.at[xx, ao], relay.at[side, n], sc.at[xx, ao], rf.at[side, n], to).start()
        remote(scales.at[xx, ao], relay_s.at[side, n], ss.at[xx, ao], rfs.at[side, n], to).start()

    def hand_on(o, wait_only=False):
        side, n = o % 2, o // 2
        xx = (pb, bl, br, bo)[o]
        origin, to = (al, ar) if side == 0 else (ar, al)
        one = remote(relay.at[side, n], R.at[xx, origin], sf.at[side, n], rf.at[side, n], along("a", to))
        one.wait_recv()
        two = remote(relay_s.at[side, n], RS.at[xx, origin], sfs.at[side, n], rfs.at[side, n], along("a", to))
        two.wait_recv()
        remote(relay.at[side, n], R.at[xx, origin], sf.at[side, n], rc.at[xx, origin], along("a", to)).start()
        remote(relay_s.at[side, n], RS.at[xx, origin], sfs.at[side, n], rs.at[xx, origin], along("a", to)).start()

    locals_[0].wait()
    locals_[1].wait()
    unit(pb, pa, R.at[pb, pa], RS.at[pb, pa])
    locals_[2].wait()
    locals_[3].wait()
    rank = rft.shape[0]
    r_high, r_low = split(rfv[...])
    R2[0:rank] = r_high
    R2[rank : 2 * rank] = r_low
    LT[...] = jnp.zeros_like(LT)

    def mom_left(g, carry):
        r = cols_of(g * 256, 256)
        high, low = split(both[:, r])
        v = dot(R2[:, r], high, ((1,), (1,)))
        LT[...] += v[0:rank] + v[rank:] + dot(R2[0:rank, r], low, ((1,), (1,)))
        return carry

    lax.fori_loop(0, both.shape[1] // 256, mom_left, 0)

    got_a(0)
    pass_a(4, 0, al, ar)
    got_a(3)
    pass_a(5, 1, ar, al)
    got_b(0)
    pass_b(4, 0, bl, br)
    got_b(3)
    pass_b(5, 1, br, bl)
    got_a(1)
    got_a(2)

    def own_cols(i, carry):
        zz = around(pa, 3 - 2 * i)
        made(pb, zz)
        home(pb, zz)
        return carry

    lax.fori_loop(0, 2, own_cols, 0)
    got_b(1)
    got_b(2)

    def next_cols(i, carry):
        xx = around(pb, 3 - 2 * lax.div(i, 3))
        m = lax.rem(i, 3)

        @pl.when(m == 2)
        def _():
            unit(xx, pa, R.at[xx, pa], RS.at[xx, pa])

        @pl.when(m != 2)
        def _():
            made(xx, around(pa, 3 - 2 * m))

        return carry

    lax.fori_loop(0, 6, next_cols, 0)
    got_a(4)
    got_a(5)

    def far_rows(i, carry):
        xx = around(pb, jnp.where(i == 0, 0, 5 - 2 * i))
        made(xx, ao)
        half_way(xx, lax.rem(i, 2), lax.div(i, 2))
        return carry

    lax.fori_loop(0, 3, far_rows, 0)
    for xx in (bl, br):
        home(xx, al)
        home(xx, ar)
    for o in range(3):
        hand_on(o)
    got_b(4)
    got_b(5)

    def far_cols(i, carry):
        @pl.when(i == 0)
        def _():
            made(bo, ao)
            half_way(bo, 1, 1)

        @pl.when(jnp.logical_and(i != 0, i != 3))
        def _():
            zz = around(pa, 5 - 2 * i)
            made(bo, zz)
            home(bo, zz)

        @pl.when(i == 3)
        def _():
            unit(bo, pa, R.at[bo, pa], RS.at[bo, pa])

        return carry

    lax.fori_loop(0, 4, far_cols, 0)
    late, far = lax.div(bo, 2), lax.div(ao, 2)

    def gather_home(n, carry):
        o = jnp.where(n < 6, lax.rem(n, 3), 3)
        h = jnp.where(jnp.logical_or(n < 3, n == 6), 1 - far, far)
        xx = around(pb, jnp.where(o == 0, 0, jnp.where(o == 3, 2, 5 - 2 * o)))
        group = jnp.where(n < 4, 1 - late, late)
        m = lax.rem(n, 4)
        zz = around(pa, jnp.where(m == 0, 0, jnp.where(m == 3, 2, 5 - 2 * m)))
        base = jnp.where(c == 0, xx * 2 + h, zz * 2 + group) * (2 * feats)
        for i in range(2):
            xi = jnp.where(c == 0, xx, 2 * group + i)
            zi = jnp.where(c == 0, 2 * h + i, zz)

            @pl.when(zi != pa)
            def _():
                remote(codes.at[0, 0], R.at[xi, zi], sc.at[0, 0], rc.at[xi, zi], along("a", ar)).wait_recv()
                remote(scales.at[0, 0], RS.at[xi, zi], ss.at[0, 0], rs.at[xi, zi], along("a", ar)).wait_recv()

            S[i * feats : (i + 1) * feats] = R[xi, zi].astype(jnp.int32).astype(f32) * RS[xi, zi, 0:1]
        high, low = split(S[...])
        r = cols_of(base, 2 * feats)
        v = dot(R2[:, r], high)
        LT[...] += v[0:rank] + v[rank:] + dot(R2[0:rank, r], low)
        for i in range(2 * feats // 128):
            both[:, cols_of(base + 128 * i, 128)] += S[128 * i : 128 * (i + 1)].T
        return carry

    lax.fori_loop(0, 3, gather_home, 0)
    hand_on(3)
    lax.fori_loop(3, 8, gather_home, 0)

    pending = []

    def swap(stage, src, dst, k=0):
        copy = remote(src, dst, send.at[stage, k], recv.at[stage, k], mate)
        copy.start()
        pending.append(copy)
        return copy

    def spread(stage, axis, src, dst):
        me = place[axis]
        waits = []
        for q in (2, 1, 3):
            k = around(me, q)
            copy = remote(src(k), dst(me), send.at[stage, q], recv.at[stage, q], along(axis, k))
            copy.start()
            pending.append(copy)
            waits.append(remote(src(k), dst(around(me, 4 - q)), send.at[stage, q], recv.at[stage, q], along(axis, k)))

        def wait():
            for w in waits:
                w.wait_recv()

        return wait

    swap(0, LT, L0).wait_recv()
    L1[y] = LT[...] + L0[...]
    spread(1, "y", lambda k: L1.at[y], lambda k: L1.at[k])()
    left = (L1[0] + L1[1] + L1[2] + L1[3]) * (1.0 / 8.0)
    left_high, left_low = split(left)
    LL[0:rank] = left_high
    LL[rank : 2 * rank] = left_low
    v = dot(LL[...], left_high, ((1,), (1,)))
    G1[z] = v[0:rank] + v[rank:] + dot(left_high, left_low, ((1,), (1,)))
    gram_wait = spread(2, "z", lambda k: G1.at[z], lambda k: G1.at[k])

    tiles = both.shape[1] // 128 * (rank // 8)
    half = tiles // 2
    blocks = both.shape[1] // 512

    def block(g, carry):
        high, low = split(both[:, cols_of(g * 256, 256)])
        v = dot(LL[...], high)
        v = v[0:rank] + v[rank:] + dot(LL[0:rank], low)
        for i in range(2):
            T[pl.ds(g * 16 + i * 8, 8)] = v[:, 128 * i : 128 * (i + 1)].reshape(8, 8, 128)
        return carry

    orders = (("y", "x", "z"), ("x", "z", "y"), ("z", "y", "x"))
    sizes = parts_of(half)
    begin = (0, sizes[0], sizes[0] + sizes[1])
    mine, theirs = c * half, (1 - c) * half
    base = [mine + start for start in begin]
    n1 = [size // 4 for size in sizes]
    n2 = [size // 16 for size in sizes]

    def part_blocks(side, k):
        start = blocks * side + begin[k] // 16
        return start, start + sizes[k] // 16

    core_waits = []
    for k in range(3):
        lax.fori_loop(*part_blocks(1 - c, k), block, 0)
        core_waits.append(
            swap(3, T.at[pl.ds(theirs + begin[k], sizes[k])], D.at[pl.ds(begin[k], sizes[k])], k)
        )

    def add_core(g, carry):
        r = pl.ds(mine + g * 16, 16)
        T[r] = T[r] + D[pl.ds(g * 16, 16)]
        return carry

    zeroth, first, second, third, fourth = [], [], [], [], []
    for k, (a1, a2, a3) in enumerate(orders):
        lax.fori_loop(*part_blocks(c, k), block, 0)
        core_waits[k].wait_recv()
        lax.fori_loop(begin[k] // 16, (begin[k] + sizes[k]) // 16, add_core, 0)
        zeroth.append(
            spread(
                4 + k, a1,
                lambda q, k=k: T.at[pl.ds(base[k] + q * n1[k], n1[k])],
                lambda q, k=k: P1.at[k, q, 0 : n1[k]],
            )
        )
    gram_wait()
    G2[x] = G1[0] + G1[1] + G1[2] + G1[3]
    gram_wait = spread(19, "x", lambda k: G2.at[x], lambda k: G2.at[k])
    for k, (a1, a2, a3) in enumerate(orders):
        me = place[a1]
        P1[k, me, 0 : n1[k]] = T[pl.ds(base[k] + me * n1[k], n1[k])]
        zeroth[k]()
        low = slice(0, n1[k])
        P1[k, 0, low] = P1[k, 0, low] + P1[k, 1, low] + P1[k, 2, low] + P1[k, 3, low]
        first.append(
            spread(
                7 + k, a2,
                lambda q, k=k: P1.at[k, 0, pl.ds(q * n2[k], n2[k])],
                lambda q, k=k: P2.at[k, q, 0 : n2[k]],
            )
        )
    row_id = lax.broadcasted_iota(jnp.int32, (rank, 2 * rank), 0)
    lane_id = lax.broadcasted_iota(jnp.int32, (rank, 2 * rank), 1)
    gram_wait()
    M[...] = jnp.where(lane_id == row_id + rank, 1.0, 0.0)
    M[:, 0:rank] = G2[0] + G2[1] + G2[2] + G2[3]

    def pivot(k, carry):
        m = M[...]
        row = M[pl.ds(k, 1), :]
        top = jnp.sum(jnp.where(lane_id[0:1] == k, row, 0.0), axis=1, keepdims=True)
        factor = jnp.sum(jnp.where(lane_id == k, m, 0.0), axis=1, keepdims=True)
        factor = jnp.where(row_id[:, 0:1] > k, factor / top, 0.0)
        M[...] = m - factor * row
        return carry

    cuts = (0, 16, 32, 48, rank)
    lax.fori_loop(cuts[0], cuts[1], pivot, 0)
    for k, (a1, a2, a3) in enumerate(orders):
        me = place[a2]
        low = slice(0, n2[k])
        P2[k, me, low] = P1[k, 0, pl.ds(me * n2[k], n2[k])]
        first[k]()
        m3 = place[a3]
        P3[k, m3, low] = P2[k, 0, low] + P2[k, 1, low] + P2[k, 2, low] + P2[k, 3, low]
        second.append(
            spread(
                10 + k, a3,
                lambda q, k=k, m3=m3: P3.at[k, m3, 0 : n2[k]],
                lambda q, k=k: P3.at[k, q, 0 : n2[k]],
            )
        )
    lax.fori_loop(cuts[1], cuts[2], pivot, 0)
    for k, (a1, a2, a3) in enumerate(orders):
        second[k]()
        row = base[k] + place[a1] * n1[k]
        spot = row + place[a2] * n2[k]
        low = slice(0, n2[k])
        out[pl.ds(spot, n2[k])] = P3[k, 0, low] + P3[k, 1, low] + P3[k, 2, low] + P3[k, 3, low]
        third.append(
            spread(
                13 + k, a2,
                lambda q, spot=spot, k=k: out.at[pl.ds(spot, n2[k])],
                lambda q, row=row, k=k: out.at[pl.ds(row + q * n2[k], n2[k])],
            )
        )
    lax.fori_loop(cuts[2], cuts[3], pivot, 0)
    for k, (a1, a2, a3) in enumerate(orders):
        third[k]()
        row = base[k] + place[a1] * n1[k]
        fourth.append(
            spread(
                16 + k, a1,
                lambda q, row=row, k=k: out.at[pl.ds(row, n1[k])],
                lambda q, k=k: out.at[pl.ds(base[k] + q * n1[k], n1[k])],
            )
        )
    lax.fori_loop(cuts[3], cuts[4], pivot, 0)
    m = M[...]
    diag = jnp.sum(jnp.where(lane_id == row_id, m, 0.0), axis=1, keepdims=True)
    linv = pltpu.roll(m / jnp.sqrt(diag), rank, 1)[:, 0:rank]
    ortho_out[...] = jnp.dot(linv, (L1[0] + L1[1] + L1[2] + L1[3]) * (1.0 / 8.0), precision=HI, preferred_element_type=f32)
    v_high, v_low = split(linv * (1.0 / 8.0))
    LV[0] = v_high
    LV[1] = v_low
    for k in range(3):
        fourth[k]()
        r = pl.ds(base[k], sizes[k])
        swap(20, out.at[r], out.at[r], k)

    def right(j, sq):
        high, low = split(jnp.concatenate([tile_column(out, 2 * j), tile_column(out, 2 * j + 1)], axis=1))
        v = dot(LV[0], high) + dot(LV[1], high) + dot(LV[0], low)
        RT[:, cols_of(j * 256, 256)] = v
        return sq + v * v

    sq = jnp.zeros((rank, 256), f32)
    sq_other = sq
    for k in range(3):
        sq = lax.fori_loop(*part_blocks(c, k), right, sq)
    for k in range(3):
        r = pl.ds(theirs + begin[k], sizes[k])
        remote(out.at[r], out.at[r], send.at[20, k], recv.at[20, k], mate).wait_recv()
        sq_other = lax.fori_loop(*part_blocks(1 - c, k), right, sq_other)
    total = jnp.where(c == 0, sq, sq_other) + jnp.where(c == 0, sq_other, sq)
    norm = lax.rsqrt(jnp.sum(total, axis=1, keepdims=True) + EPS)
    norm_out[...] = jnp.broadcast_to(norm, norm_out.shape)

    for copy in pending + sent:
        copy.wait_send()
    for by in (1, 2, 3):
        for xx in range(4):
            zz = around(pa, by)
            remote(codes.at[xx, zz], R.at[0, 0], sc.at[xx, zz], rc.at[0, 0], along("a", ar)).wait_send()
            remote(scales.at[xx, zz], RS.at[0, 0], ss.at[xx, zz], rs.at[0, 0], along("a", ar)).wait_send()
    for o in range(4):
        side, n = o % 2, o // 2
        remote(relay.at[side, n], R.at[0, 0], sf.at[side, n], rc.at[0, 0], along("a", ar)).wait_send()
        remote(relay_s.at[side, n], RS.at[0, 0], sfs.at[side, n], rs.at[0, 0], along("a", ar)).wait_send()


def communicate(cot, bt, lengths, mom, rft):
    tok, rows = cot.shape
    feats = bt.shape[0]
    rank, cols = rft.shape
    tiles = cols // 128 * (rank // 8)
    half = tiles // 2
    most = max(parts_of(half))
    n1, n2 = most // 4, most // 16
    return pl.pallas_call(
        comm_kernel,
        out_shape=(
            jax.ShapeDtypeStruct((rows, cols), f32),
            jax.ShapeDtypeStruct((rank, cols), f32),
            jax.ShapeDtypeStruct((rank, 128), f32),
            jax.ShapeDtypeStruct((rank, rows), f32),
        ),
        in_specs=[hspec(), hspec(), sspec(), hspec(), hspec()],
        out_specs=(vspec(), vspec(), vspec(), vspec()),
        scratch_shapes=[
            VMEM((4, tok, rows), bf16),
            VMEM((4, feats, tok), bf16),
            VMEM((4, 4, feats, rows), jnp.int16),
            VMEM((4, 4, 8, rows), f32),
            VMEM((4, 4, feats, rows), jnp.int16),
            VMEM((4, 4, 8, rows), f32),
            VMEM((2, 2, feats, rows), jnp.int16),
            VMEM((2, 2, 8, rows), f32),
            VMEM((feats, rows), f32),
            VMEM((16, tok), bf16),
            VMEM((2 * feats, rows), f32),
            VMEM((2 * rank, cols), bf16),
            VMEM((rank, cols), f32),
            VMEM((rank, rows), f32),
            VMEM((rank, rows), f32),
            VMEM((4, rank, rows), f32),
            VMEM((2 * rank, rows), bf16),
            VMEM((2, rank, rank), bf16),
            VMEM((tiles, 8, 128), f32),
            VMEM((half, 8, 128), f32),
            VMEM((tiles, 8, 128), f32),
            VMEM((3, 4, n1, 8, 128), f32),
            VMEM((3, 4, n2, 8, 128), f32),
            VMEM((3, 4, n2, 8, 128), f32),
            VMEM((4, rank, rank), f32),
            VMEM((4, rank, rank), f32),
            VMEM((rank, 2 * rank), f32),
            DMA((5,)), DMA((6,)), DMA((6,)), DMA((6,)), DMA((6,)),
            DMA((4, 4)), DMA((4, 4)), DMA((4, 4)), DMA((4, 4)),
            DMA((2, 2)), DMA((2, 2)), DMA((2, 2)), DMA((2, 2)),
            DMA((21, 4)), DMA((21, 4)),
        ],
        compiler_params=pltpu.CompilerParams(
            collective_id=0, has_side_effects=True, vmem_limit_bytes=COMM_BYTES
        ),
        name="communicate",
    )(cot, bt, lengths, mom, rft)


def finish_kernel(
    coef, right_t, norm, ortho_t, both, weight, new_weight, new_mom, new_right_t,
    bv, wv, NR, O3, osem,
):
    rows, cols = both.shape
    wide = cols // 8

    def store(i):
        r = cols_of(i * wide, wide)
        return (
            pltpu.make_async_copy(bv.at[:, r], new_mom.at[:, r], osem.at[i, 0]),
            pltpu.make_async_copy(wv.at[:, r], new_weight.at[:, r], osem.at[i, 1]),
            pltpu.make_async_copy(NR.at[:, r], new_right_t.at[:, r], osem.at[i, 2]),
        )

    both_t = jnp.concatenate([ortho_t[...] * (1.0 - MU), ortho_t[...] * (norm[:, 0:1] * coef)], axis=1)
    o_high, o_low = split(both_t)
    O3[...] = jnp.concatenate([o_high, o_high, o_low], axis=0).T

    def work(i, carry):
        r = cols_of(i * wide, wide)
        v = right_t[:, r]
        high, low = split(v)
        change = dot(O3[...], jnp.concatenate([high, low, high], axis=0))
        bv[:, r] = both[:, r] - change[0:rows]
        wv[:, r] = (weight[:, r].astype(f32) - change[rows:]).astype(bf16)
        NR[:, r] = v * norm[:, 0:1]
        for copy in store(i):
            copy.start()
        return carry

    lax.fori_loop(0, 8, work, 0)
    for i in range(8):
        for copy in store(i):
            copy.wait()


def finish(coef, right_t, norm, ortho_t, both, weight):
    rows, cols = both.shape
    rank = right_t.shape[0]
    return pl.pallas_call(
        functools.partial(finish_kernel, coef),
        out_shape=(
            jax.ShapeDtypeStruct((rows, cols), bf16),
            jax.ShapeDtypeStruct((rows, cols), f32),
            jax.ShapeDtypeStruct((rank, cols), f32),
        ),
        in_specs=[vspec()] * 5,
        out_specs=(hspec(), hspec(), hspec()),
        scratch_shapes=[
            VMEM((rows, cols), f32),
            VMEM((rows, cols), bf16),
            VMEM((rank, cols), f32),
            VMEM((2 * rows, 3 * rank), bf16),
            DMA((8, 3)),
        ],
        compiler_params=pltpu.CompilerParams(vmem_limit_bytes=FINISH_BYTES),
        name="finish",
    )(right_t, norm, ortho_t, both, weight)


def per_device(inputs, cotangent, lengths, momentum, weight, right_factor):
    stay = lambda v: pltpu.with_memory_space_constraint(v, pltpu.HBM)
    both, right_t, norm, ortho_t = communicate(
        stay(cotangent), stay(inputs.T), stay(lengths), stay(momentum[0]), stay(right_factor.T)
    )
    rows_all = both.shape[0] * lax.axis_size("tensor")
    coef = LR * math.sqrt(rows_all / both.shape[1])
    new_weight, new_mom, new_right_t = finish(coef, right_t, norm, ortho_t, both, weight)
    return (new_weight, new_mom[None], new_right_t.T)


def solution(mesh):
    placed = (
        P("dp", "tensor"),
        P("dp", "tensor"),
        P("dp"),
        P("dp", "tensor", None),
        P("tensor", None),
        P(),
    )
    return jax.shard_map(
        per_device,
        mesh=mesh,
        in_specs=placed,
        out_specs=(P("tensor", None), P("dp", "tensor", None), P()),
        check_vma=False,
    )
```
